512 devices in a mesh: freq: 4 (over y), row: 8 (over x, core), col: 16 (over z).
Axes of the slice: x: 4, y: 4, z: 16, core: 2. Of those that a mesh axis runs over, the one named last changes fastest.
Arguments:
- snapshots: bfloat16 [32, 1024, 128], P('freq', 'col'), may hold values from -60 to 60, as said below
- replicas: bfloat16 [32, 2, 1024, 8192], P('freq', None, 'col', 'row'), may hold values from -64 to 64, as said below
- level_index: int32 [32], P('freq'), may hold values from 0 to 7
- loading_iters: int32 [32], P('freq'), may hold values from 1 to 2
Outputs:
- log_power: float32 [32, 8192], P('freq', ('row', 'col'))
- broadband: float32 [8192], P(('row', 'col'))
The draws below stay inside these ranges and needn't reach their ends.
Inputs may be any that keep to these rules, and one draw needn't show every extreme that they name: `snapshots`: each frequency's snapshots are independent of the other frequencies' snapshots. `replicas`: each candidate's field is sensor noise plus a part in the span of its frequency's snapshots.
All inputs are finite; a program needn't handle non-finite values.
Results may differ from the reference program's by a relative error of at most 0.0003.
Values may be sent and summed in bfloat16 or wider, within the bound.
A program may use at most 64 MiB of HBM per device.

```python
import math
import jax
import jax.numpy as jnp
from jax import lax

M = 1024
K = 64
LEVELS = 8
FREQS = 32
CANDS = 8192


def make_fields(key):
    base = jax.random.fold_in(key, 91)
    keys = jax.random.split(base, 4)
    snaps = jax.random.normal(keys[0], (FREQS, M, 2 * K), jnp.float32)
    noise = jax.random.normal(keys[1], (FREQS, 2, M, CANDS), jnp.float32)
    mixing = jax.random.normal(keys[2], (FREQS, 2 * K, CANDS), jnp.float32) / math.sqrt(K)
    real_snap = snaps[:, :, :K]
    imag_snap = snaps[:, :, K:]
    real_mix = mixing[:, :K, :]
    imag_mix = mixing[:, K:, :]
    real_field = jnp.einsum('fmk,fkc->fmc', real_snap, real_mix) - jnp.einsum('fmk,fkc->fmc', imag_snap, imag_mix)
    imag_field = jnp.einsum('fmk,fkc->fmc', real_snap, imag_mix) + jnp.einsum('fmk,fkc->fmc', imag_snap, real_mix)
    ramp = 0.3 + 2.7 * jnp.arange(CANDS).astype(jnp.float32) / CANDS
    spread = jnp.exp(jax.random.uniform(keys[3], (CANDS,), jnp.float32, 0.0, math.log(3.0)))
    strength = (ramp * spread)[None, None, None, :]
    reps = noise + strength * jnp.stack([real_field, imag_field], 1)
    return (jnp.clip(snaps, -60.0, 60.0), jnp.clip(reps, -64.0, 64.0))


def draw_snapshots(key, part):
    return make_fields(key)[0].astype(jnp.bfloat16)


def draw_replicas(key, part):
    return make_fields(key)[1].astype(jnp.bfloat16)


def with_ends(drawn, stream_key, least, high):
    extent = drawn.shape
    spot = [jax.random.randint(jax.random.fold_in(stream_key, axis), (), 0, extent[axis]) for axis in range(len(extent))]
    drawn = drawn.at[tuple(spot)].set(least)
    longest = extent.index(max(extent))
    spot[longest] = (spot[longest] + 1) % extent[longest]
    return drawn.at[tuple(spot)].set(high)


def setup_inputs(seed: int = 0) -> dict:
    key_of = jax.random.split(jax.random.key(seed), 5)
    snapshots = draw_snapshots(jax.random.fold_in(key_of[4], 71), 0)
    replicas = draw_replicas(jax.random.fold_in(key_of[4], 71), 0)
    level_index = with_ends(jax.random.randint(key_of[2], (FREQS,), 0, LEVELS), jax.random.fold_in(key_of[2], 1), 0, LEVELS - 1).astype(jnp.int32)
    loading_iters = with_ends(jax.random.randint(key_of[3], (FREQS,), 1, 3), jax.random.fold_in(key_of[3], 1), 1, 2).astype(jnp.int32)
    return {"snapshots": snapshots, "replicas": replicas, "level_index": level_index, "loading_iters": loading_iters}


gain_target = 0.5

def stack_snapshots(snaps):
    count = snaps.shape[-1] // 2
    real_part = snaps[..., :count]
    imag_part = snaps[..., count:]
    upper = jnp.concatenate([real_part, -imag_part], -1)
    lower = jnp.concatenate([imag_part, real_part], -1)
    return jnp.concatenate([upper, lower], -2)

def sensor_products(items):
    snaps, reps = items
    stacked = stack_snapshots(snaps).astype(jnp.float32)
    columns = reps.reshape(2 * reps.shape[1], reps.shape[2]).astype(jnp.float32)
    projected = jnp.dot(stacked.T.astype(jnp.float32), columns.astype(jnp.float32), precision=lax.Precision.HIGHEST, preferred_element_type=jnp.float32)
    gram_raw = jnp.dot(stacked.T.astype(jnp.float32), stacked.astype(jnp.float32), precision=lax.Precision.HIGHEST, preferred_element_type=jnp.float32)
    norms = lax.optimization_barrier(jnp.sum(columns * columns, 0))
    return (projected, gram_raw, norms)

def prepare(projected, gram_raw, level_index):
    snap_count = gram_raw.shape[1] // 2
    gram = gram_raw / snap_count
    proj = projected * (1.0 / math.sqrt(snap_count))
    power = jnp.trace(gram, axis1=1, axis2=2) / (2.0 * M)
    steps = jnp.arange(LEVELS).astype(jnp.int32)
    levels = 2.0 ** (steps.astype(jnp.float32) / 2.0)
    chosen = lax.optimization_barrier(jnp.sum(jnp.where(steps[None, :] == level_index[:, None], levels[None, :], 0.0), 1))
    return (gram, proj, power, chosen * power)

def loading_pass(gram, proj, replica_norm, loading):
    dimension = gram.shape[1]
    identity = jnp.eye(dimension, dtype=gram.dtype)
    system = loading[:, None, None] * identity + gram

    def invert(matrix):
        factor = jnp.linalg.cholesky(matrix)
        return jax.scipy.linalg.cho_solve((factor, True), identity)
    inverse = jax.vmap(invert)(system)
    solved = jnp.einsum('fkl,flc->fkc', inverse, proj, precision=lax.Precision.HIGHEST)
    inner_sum = lax.optimization_barrier(jnp.sum(proj * solved, 1))
    energy = lax.optimization_barrier(jnp.sum(solved * solved, 1))
    quad_one = (replica_norm - inner_sum) / loading[:, None]
    quad_two = (quad_one - energy) / loading[:, None]
    return (quad_one, quad_two)

def reference(snapshots, replicas, level_index, loading_iters):
    projected, gram_raw, replica_norm = lax.map(sensor_products, (snapshots, replicas))
    gram, proj, power, loading_one = prepare(projected, gram_raw, level_index)
    quad_one, quad_two = loading_pass(gram, proj, replica_norm, loading_one)
    gains = quad_one * quad_one / (quad_two * replica_norm)
    mean_gain = lax.optimization_barrier(jnp.sum(gains, 1)) / CANDS
    loading_two = loading_one * (1.0 + (gain_target / mean_gain) ** 2)
    quad_next, unused = loading_pass(gram, proj, replica_norm, loading_two)
    final = jnp.where(loading_iters[:, None] >= 2, quad_next, quad_one)
    log_power = jnp.log(replica_norm / (final * power[:, None]))
    broadband = lax.optimization_barrier(jnp.sum(log_power, 0)) / FREQS
    return (log_power, broadband)
```

```python
import functools

import jax
import jax.numpy as jnp
from jax import lax
from jax.experimental import pallas as pl
from jax.experimental.pallas import tpu as pltpu
from jax.sharding import PartitionSpec as P

SENSORS = 1024
SNAPS = 64
LEVELS = 8
LANES = 128
HALF = 64
GAIN_TARGET = 0.5
MESH_ID = pl.DeviceIdType.MESH
F32 = jnp.float32


def kernel(
    nf, nr, nz,
    lvl_ref, it_ref, snaps_ref, reps_ref,
    logp_ref, band_ref,
    part, recv, gp, grecv, gall, gram, gain_z, gain_r, band_b,
    rs_s, rs_r, ga_s, ga_r, gb_s, gb_r, gc_s, gc_r, qz_s, qz_r, qr_s, qr_r, fb_s, fb_r,
    *mats,
):
    freqs = nr
    pairs = freqs // 2
    hops = nz // 2
    piece = HALF // nz
    me_f, me_r, me_z = lax.axis_index("freq"), lax.axis_index("row"), lax.axis_index("col")
    lane = lax.broadcasted_iota(jnp.int32, (1, LANES), 1)
    low = lane < HALF
    sign_hi = jnp.where(low, 1.0, -1.0).astype(F32)
    sign_lo = jnp.where(low, -1.0, 1.0).astype(F32)
    rows64 = lax.broadcasted_iota(jnp.int32, (HALF, LANES), 0)
    lanes64 = lax.broadcasted_iota(jnp.int32, (HALF, LANES), 1)
    eye = rows64 == lanes64

    def ahead(me, step, count):
        return lax.rem(me + (step + count), count)

    def remote(src, dst, send, got, axis, peer):
        return pltpu.make_async_remote_copy(
            src_ref=src, dst_ref=dst, send_sem=send, recv_sem=got,
            device_id={axis: peer}, device_id_type=MESH_ID,
        )

    barrier = pltpu.get_barrier_semaphore()
    for axis, me, count in (("col", me_z, nz), ("row", me_r, nr), ("freq", me_f, nf)):
        for o in range(1, count):
            pl.semaphore_signal(barrier, inc=1, device_id={axis: ahead(me, o, count)}, device_id_type=MESH_ID)

    x = snaps_ref[me_r]
    w = lax.dot_general(x, x, (((0,), (0,)), ((), ())), preferred_element_type=F32)
    w_up, w_down = w[:HALF, :], w[HALF:, :]
    turned = pltpu.roll(w_down, HALF, 1)
    compact = w_up + turned * sign_hi
    for j in range(nz):
        gp[j] = compact[j * piece:(j + 1) * piece, :]

    for s in range(pairs):
        prods, norms = [], []
        for f in (2 * s, 2 * s + 1):
            snap = snaps_ref[f].astype(F32)
            stacked = jnp.concatenate([snap * sign_hi, pltpu.roll(snap, HALF, 1)], axis=0)
            cols = reps_ref[f]
            prods.append(jnp.dot(stacked.T.astype(jnp.bfloat16), cols, preferred_element_type=F32))
            wide = cols.astype(F32)
            norms.append(jnp.sum(wide * wide, axis=0, keepdims=True))
        for m in range(nz // 2):
            at = slice(m * LANES, (m + 1) * LANES)
            for pair, top, count in ((prods, s * LANES, LANES), (norms, pairs * LANES + s, 1)):
                a, b = pair[0][:, at], pair[1][:, at]
                part[2 * m, top:top + count, :] = jnp.where(low, a, pltpu.roll(b, HALF, 1))
                part[2 * m + 1, top:top + count, :] = jnp.where(low, pltpu.roll(a, HALF, 1), b)
    for d in range(nz):
        part[d, pairs * LANES + pairs:, :] = jnp.zeros((8 - pairs, LANES), F32)

    pl.semaphore_wait(barrier, (nz - 1) + (nr - 1) + (nf - 1))
    pending = []

    ga = []
    for o in range(1, nz):
        to = ahead(me_z, o, nz)
        c = remote(gp.at[to], grecv.at[me_z], ga_s.at[o], ga_r.at[o], "col", to)
        c.start()
        ga.append(c)

    def gram_second():
        total = gp[me_z]
        for o in range(1, nz):
            ga[o - 1].wait_recv()
        for o in range(1, nz):
            total = total + grecv[ahead(me_z, -o, nz)]
        pending.extend(ga)
        gall[me_r, me_z] = total
        for o in range(1, nz):
            c = remote(gall.at[me_r, me_z], gall.at[me_r, me_z], gb_s.at[o], gb_r.at[o], "col", ahead(me_z, o, nz))
            c.start()
            gb.append(c)

    gb, gc = [], []

    def gram_third():
        for c in gb:
            c.wait_recv()
        pending.extend(gb)
        for o in range(1, nr):
            c = remote(gall.at[me_r], gall.at[me_r], gc_s.at[o], gc_r.at[o], "row", ahead(me_r, o, nr))
            c.start()
            gc.append(c)

    powers, loads_one = [], []

    def set_system(f, load):
        mats[f][...] = gram[f] + jnp.where(eye, load, 0.0)

    def gram_done():
        for c in gc:
            c.wait_recv()
        pending.extend(gc)
        for f in range(freqs):
            for j in range(nz):
                gram[f, j * piece:(j + 1) * piece, :] = gall[f, j] * (1.0 / SNAPS)
        for f in range(freqs):
            diag = jnp.sum(jnp.where(eye, gram[f], 0.0), axis=0, keepdims=True)
            power = 2.0 * jnp.sum(diag, axis=1, keepdims=True) / (2.0 * SENSORS)
            level = lvl_ref[f]
            chosen = jnp.float32(0.0)
            for n in range(LEVELS):
                chosen = jnp.where(level == n, jnp.float32(2.0 ** (n / 2.0)), chosen)
            powers.append(power)
            loads_one.append(chosen * power)
            set_system(f, loads_one[f])

    def sweep(first, last):
        def one(k, carry):
            at_re = lane == k
            at_im = lane == k + HALF
            either = at_re | at_im
            ups, turns, res, ims, tiles = [], [], [], [], []
            for f in range(freqs):
                row = mats[f][pl.ds(k, 1), :]
                tile = mats[f][...]
                res.append(jnp.sum(jnp.where(at_re, tile, 0.0), axis=1, keepdims=True))
                ims.append(jnp.sum(jnp.where(at_im, tile, 0.0), axis=1, keepdims=True))
                pivot = jnp.sum(jnp.where(at_re, row, 0.0), axis=1, keepdims=True)
                up = jnp.where(at_re, -1.0, jnp.where(at_im, 0.0, row))
                turn = pltpu.roll(up, HALF, 1) * sign_lo
                inv = 1.0 / pivot
                ups.append(up * inv)
                turns.append(turn * inv)
            for f in range(freqs):
                tile = jnp.where(either, 0.0, mats[f][...])
                mats[f][...] = tile - res[f] * ups[f] - ims[f] * turns[f]
                mats[f][pl.ds(k, 1), :] = ups[f]
            return carry

        lax.fori_loop(first, last, one, 0)

    def arm(s, way):
        return hops if (s < (pairs + 1) // 2) == (way == 0) else hops - 1

    def span(s):
        return slice(s * LANES, (s + 1) * LANES + (8 if s == pairs - 1 else 0))

    rs = {}

    def send(way, t, s):
        sign = 1 if way == 0 else -1
        sp = span(s)
        rows = pl.ds(sp.start, sp.stop - sp.start)
        dest = ahead(me_z, sign * (arm(s, way) - t), nz)
        if t == 0:
            src = part.at[dest, rows]
        else:
            rs[way, t - 1, s].wait_recv()
            recv[way, t - 1, sp, :] = recv[way, t - 1, sp, :] + part[dest, sp, :]
            src = recv.at[way, t - 1, rows]
        c = remote(src, recv.at[way, t, rows], rs_s.at[way, t, s], rs_r.at[way, t, s], "col", ahead(me_z, sign, nz))
        c.start()
        rs[way, t, s] = c
        pending.append(c)

    total_steps = hops * pairs
    second = min(max(1, total_steps // 8), total_steps - 1)
    third = min(max(2, total_steps * 5 // 16), total_steps - 1)
    done = max(third, total_steps // 2 - 1)
    sweeps = list(range(done + 1, total_steps - 1))
    cuts = [HALF * i // len(sweeps) for i in range(len(sweeps) + 1)] if sweeps else []
    step = 0
    for t in range(hops):
        for s in range(pairs):
            for way in (0, 1):
                if t < arm(s, way):
                    send(way, t, s)
            if step == second:
                gram_second()
            if step == third:
                gram_third()
            if step == done:
                gram_done()
            if step in sweeps:
                i = sweeps.index(step)
                sweep(cuts[i], cuts[i + 1])
            step += 1
    if not sweeps:
        sweep(0, HALF)

    proj, norm = [], []
    for s in range(pairs):
        sp = span(s)
        total = part[me_z, sp, :]
        for way in (0, 1):
            last = arm(s, way) - 1
            rs[way, last, s].wait_recv()
            total = total + recv[way, last, sp, :]
        proj.append(total[:LANES] * (1.0 / 8.0))
    extra = total[LANES:]
    for s in range(pairs):
        norm.append(extra[s:s + 1, :])

    def by_half(values, s):
        return jnp.where(low, values[2 * s], values[2 * s + 1])

    def solve(s):
        got = []
        for f in (2 * s, 2 * s + 1):
            inverse = -mats[f][...]
            full = jnp.concatenate([inverse * sign_hi, pltpu.roll(inverse, HALF, 1)], axis=0)
            got.append(jnp.dot(full, proj[s], precision=lax.Precision.HIGHEST, preferred_element_type=F32))
        z = jnp.where(low, got[0], got[1])
        return (
            jnp.sum(proj[s] * z, axis=0, keepdims=True),
            jnp.sum(z * z, axis=0, keepdims=True),
        )

    ones = []
    mine = jnp.zeros((1, LANES), F32)
    for s in range(pairs):
        inner, energy = solve(s)
        load = by_half(loads_one, s)
        quad_one = (norm[s] - inner) / load
        quad_two = (quad_one - energy) / load
        gains = quad_one * quad_one / (quad_two * norm[s])
        left = jnp.sum(jnp.where(low, gains, 0.0), axis=1, keepdims=True)
        right = jnp.sum(jnp.where(low, 0.0, gains), axis=1, keepdims=True)
        mine = mine + jnp.where(lane == 2 * s, left, 0.0) + jnp.where(lane == 2 * s + 1, right, 0.0)
        ones.append(quad_one)

    def everyone(buf, me, count, axis, send_sem, recv_sem, value):
        buf[me] = value
        copies = []
        for o in range(1, count):
            c = remote(buf.at[me], buf.at[me], send_sem.at[o], recv_sem.at[o], axis, ahead(me, o, count))
            c.start()
            copies.append(c)
        for c in copies:
            c.wait_recv()
        pending.extend(copies)
        total = buf[0]
        for i in range(1, count):
            total = total + buf[i]
        return total

    whole = everyone(gain_z, me_z, nz, "col", qz_s, qz_r, mine)
    whole = everyone(gain_r, me_r, nr, "row", qr_s, qr_r, whole)
    mean_gain = whole / (HALF * nz * nr)
    for f in range(freqs):
        mean = jnp.sum(jnp.where(lane == f, mean_gain, 0.0), axis=1, keepdims=True)
        ratio = GAIN_TARGET / mean
        set_system(f, loads_one[f] * (1.0 + ratio * ratio))
    loads_two = []
    for f in range(freqs):
        mean = jnp.sum(jnp.where(lane == f, mean_gain, 0.0), axis=1, keepdims=True)
        ratio = GAIN_TARGET / mean
        loads_two.append(loads_one[f] * (1.0 + ratio * ratio))
    sweep(0, HALF)

    band = jnp.zeros((1, LANES), F32)
    for s in range(pairs):
        inner, _ = solve(s)
        quad_next = (norm[s] - inner) / by_half(loads_two, s)
        iters = jnp.where(low, it_ref[2 * s], it_ref[2 * s + 1])
        final = jnp.where(iters >= 2, quad_next, ones[s])
        log_power = jnp.log(norm[s] / (final * by_half(powers, s)))
        other = pltpu.roll(log_power, HALF, 1)
        logp_ref[2 * s:2 * s + 1, :] = log_power[:, :HALF]
        logp_ref[2 * s + 1:2 * s + 2, :] = other[:, :HALF]
        band = band + log_power + other
    band = everyone(band_b, me_f, nf, "freq", fb_s, fb_r, band)
    band_ref[...] = band[:, :HALF] / (freqs * nf)

    for c in pending:
        c.wait_send()


def solution(mesh):
    nf, nr, nz = mesh.shape["freq"], mesh.shape["row"], mesh.shape["col"]
    pairs, hops = nr // 2, nz // 2
    rows = pairs * LANES + 8
    dma = pltpu.SemaphoreType.DMA

    def body(snapshots, replicas, level_index, loading_iters):
        freqs, sensors, cands = snapshots.shape[0], snapshots.shape[1], replicas.shape[3]
        vmem = pl.BlockSpec(memory_space=pltpu.VMEM)
        smem = pl.BlockSpec(memory_space=pltpu.SMEM)
        log_power, band = pl.pallas_call(
            functools.partial(kernel, nf, nr, nz),
            out_shape=(
                jax.ShapeDtypeStruct((freqs, HALF), F32),
                jax.ShapeDtypeStruct((1, HALF), F32),
            ),
            in_specs=[smem, smem, vmem, vmem],
            out_specs=(vmem, vmem),
            scratch_shapes=[
                pltpu.VMEM((nz, rows, LANES), F32),
                pltpu.VMEM((2, hops, rows, LANES), F32),
                pltpu.VMEM((nz, HALF // nz, LANES), F32),
                pltpu.VMEM((nz, HALF // nz, LANES), F32),
                pltpu.VMEM((nr, nz, HALF // nz, LANES), F32),
                pltpu.VMEM((nr, HALF, LANES), F32),
                pltpu.VMEM((nz, 1, LANES), F32),
                pltpu.VMEM((nr, 1, LANES), F32),
                pltpu.VMEM((nf, 1, LANES), F32),
                dma((2, hops, pairs)), dma((2, hops, pairs)),
                dma((nz,)), dma((nz,)),
                dma((nz,)), dma((nz,)),
                dma((nr,)), dma((nr,)),
                dma((nz,)), dma((nz,)),
                dma((nr,)), dma((nr,)),
                dma((nf,)), dma((nf,)),
                *[pltpu.VMEM((HALF, LANES), F32)] * nr,
            ],
            compiler_params=pltpu.CompilerParams(collective_id=0, has_side_effects=True),
            name="mvdr",
        )(level_index, loading_iters, snapshots, replicas.reshape(freqs, 2 * sensors, cands))
        return log_power, band.reshape(HALF)

    return jax.shard_map(
        body,
        mesh=mesh,
        in_specs=(P("freq", "col", None), P("freq", None, "col", "row"), P("freq"), P("freq")),
        out_specs=(P("freq", ("row", "col")), P(("row", "col"))),
        check_vma=False,
    )
```

```python
import functools

import jax
import jax.numpy as jnp
from jax import lax
from jax.experimental import pallas as pl
from jax.experimental.pallas import tpu as pltpu
from jax.sharding import PartitionSpec as P

SENSORS = 1024
SNAPS = 64
LEVELS = 8
LANES = 128
HALF = 64
EXTRA = 8
GAIN_TARGET = 0.5
MESH_ID = pl.DeviceIdType.MESH
F32 = jnp.float32


def kernel(
    nf, nr, nz,
    lvl_ref, it_ref, snaps_ref, reps_hbm,
    out_ref,
    reps, part, recv, gather, mat, gram, xsend, xrecv, gain, lsend, lrecv,
    in_sem, rs_s, rs_r, ga_s, ga_r, xx_s, xx_r, qz_s, qz_r, ll_s, ll_r,
):
    freqs = nr
    pairs = freqs // 2
    blocks = nr // 2
    hops = nz // 2
    me_f, me_r, me_z = lax.axis_index("freq"), lax.axis_index("row"), lax.axis_index("col")
    lane = lax.broadcasted_iota(jnp.int32, (1, LANES), 1)
    low = lane < HALF
    sign_hi = jnp.where(low, 1.0, -1.0).astype(F32)
    sign_lo = jnp.where(low, -1.0, 1.0).astype(F32)
    eye = lax.broadcasted_iota(jnp.int32, (HALF, LANES), 0) == lax.broadcasted_iota(jnp.int32, (HALF, LANES), 1)

    def swap(v):
        return pltpu.roll(v, HALF, 1)

    def ahead(me, step, count):
        return lax.rem(me + (step + count), count)

    def remote(src, dst, send, got, peer):
        return pltpu.make_async_remote_copy(
            src_ref=src, dst_ref=dst, send_sem=send, recv_sem=got, device_id=peer, device_id_type=MESH_ID,
        )

    barrier = pltpu.get_barrier_semaphore()
    greet = [("col", ahead(me_z, 1, nz)), ("col", ahead(me_z, -1, nz))]
    greet += [("row", ahead(me_r, o, nr)) for o in range(1, nr)]
    greet += [("freq", ahead(me_f, o, nf)) for o in range(1, nf)]
    for axis, peer in greet:
        pl.semaphore_signal(barrier, inc=1, device_id={axis: peer}, device_id_type=MESH_ID)

    fetch = []
    for s in range(pairs):
        c = pltpu.make_async_copy(reps_hbm.at[pl.ds(2 * s, 2)], reps.at[pl.ds(2 * s, 2)], in_sem.at[s])
        c.start()
        fetch.append(c)

    for s in range(pairs):
        fetch[s].wait()
        prods, norms = [], []
        for f in (2 * s, 2 * s + 1):
            snap = snaps_ref[f].astype(F32)
            stacked = jnp.concatenate([snap * sign_hi, swap(snap)], axis=0)
            cols = reps[f]
            prods.append(jnp.dot(stacked.T.astype(jnp.bfloat16), cols, preferred_element_type=F32))
            wide = cols.astype(F32)
            norms.append(jnp.sum(wide * wide, axis=0, keepdims=True))
        for m in range(nz // 2):
            at = slice(m * LANES, (m + 1) * LANES)
            for pair, top, count in ((prods, s * LANES, LANES), (norms, pairs * LANES + s, 1)):
                a, b = pair[0][:, at], pair[1][:, at]
                part[2 * m, top:top + count, :] = jnp.where(low, a, swap(b))
                part[2 * m + 1, top:top + count, :] = jnp.where(low, swap(a), b)
    for d in range(nz):
        part[d, pairs * LANES + pairs:, :] = jnp.zeros((EXTRA - pairs, LANES), F32)
    gather[me_z] = snaps_ref[me_r]

    pl.semaphore_wait(barrier, len(greet))
    pending = []

    ring = {}

    def pass_on(h):
        for way, sign, reach in ((0, 1, hops), (1, -1, hops - 1)):
            if h < reach:
                slot = ahead(me_z, -sign * h, nz)
                if h == 0:
                    src = snaps_ref.at[me_r]
                else:
                    ring[way, h - 1].wait_recv()
                    src = gather.at[slot]
                c = remote(src, gather.at[slot], ga_s.at[way, h], ga_r.at[way, h], {"col": ahead(me_z, sign, nz)})
                c.start()
                ring[way, h] = c
                pending.append(c)

    found = {}

    def gram_done():
        ring[0, hops - 1].wait_recv()
        if hops > 1:
            ring[1, hops - 2].wait_recv()
        x = gather[...].reshape(nz * HALF, LANES)
        w = lax.dot_general(x, x, (((0,), (0,)), ((), ())), preferred_element_type=F32)
        gram[...] = (w[:HALF, :] + swap(w[HALF:, :]) * sign_hi) * (1.0 / SNAPS)
        diag = jnp.sum(jnp.where(eye, gram[...], 0.0), axis=0, keepdims=True)
        power = 2.0 * jnp.sum(diag, axis=1, keepdims=True) / (2.0 * SENSORS)
        level = lvl_ref[me_r]
        chosen = jnp.float32(0.0)
        for n in range(LEVELS):
            chosen = jnp.where(level == n, jnp.float32(2.0 ** (n / 2.0)), chosen)
        found["power"] = power
        found["load"] = chosen * power
        set_system(found["load"])

    def set_system(load):
        mat[...] = gram[...] + jnp.where(eye, load, 0.0)

    def sweep(first, last):
        def at(v, where):
            return jnp.sum(jnp.where(where, v, 0.0), axis=1, keepdims=True)

        def one(i, carry):
            k = 2 * i
            re0, re1 = lane == k, lane == k + 1
            im0, im1 = lane == k + HALF, lane == k + (HALF + 1)
            pivots = re0 | re1 | im0 | im1
            tile = mat[...]
            row0, row1 = mat[pl.ds(k, 1), :], mat[pl.ds(k + 1, 1), :]
            c0r, c0i, c1r, c1i = at(tile, re0), at(tile, im0), at(tile, re1), at(tile, im1)
            a, br, bi, c = at(row0, re0), at(row0, re1), at(row0, im1), at(row1, re1)
            r0 = jnp.where(re0, -1.0, jnp.where(pivots, 0.0, row0))
            r1 = jnp.where(re1, -1.0, jnp.where(pivots, 0.0, row1))
            j0, j1 = swap(r0) * sign_lo, swap(r1) * sign_lo
            inv = 1.0 / (a * c - (br * br + bi * bi))
            ca, cc, cr, ci = a * inv, c * inv, br * inv, bi * inv
            u0 = cc * r0 - (cr * r1 + ci * j1)
            u1 = ca * r1 - (cr * r0 - ci * j0)
            w0 = cc * j0 - (cr * j1 - ci * r1)
            w1 = ca * j1 - (cr * j0 + ci * r0)
            tile = jnp.where(pivots, 0.0, tile)
            mat[...] = tile - (c0r * u0 + c0i * w0) - (c1r * u1 + c1i * w1)
            mat[pl.ds(k, 1), :] = u0
            mat[pl.ds(k + 1, 1), :] = u1
            return carry

        lax.fori_loop(first, last, one, 0)

    def arm(s, way):
        return hops if (s < (pairs + 1) // 2) == (way == 0) else hops - 1

    def span(s):
        return slice(s * LANES, (s + 1) * LANES + (EXTRA if s == pairs - 1 else 0))

    rs = {}

    def send(way, t, s):
        sign = 1 if way == 0 else -1
        sp = span(s)
        rows = pl.ds(sp.start, sp.stop - sp.start)
        dest = ahead(me_z, sign * (arm(s, way) - t), nz)
        if t == 0:
            src = part.at[dest, rows]
        else:
            rs[way, t - 1, s].wait_recv()
            recv[way, t - 1, sp, :] = recv[way, t - 1, sp, :] + part[dest, sp, :]
            src = recv.at[way, t - 1, rows]
        c = remote(src, recv.at[way, t, rows], rs_s.at[way, t, s], rs_r.at[way, t, s], {"col": ahead(me_z, sign, nz)})
        c.start()
        rs[way, t, s] = c
        pending.append(c)

    order = [pairs - 1] + list(range(pairs - 1))
    total_steps = hops * pairs
    gap = 2 if total_steps >= 4 * hops else 1
    done = min(gap * hops + 1, total_steps - 1)
    sweeps = list(range(done + 1, total_steps - 1))
    pivots = HALF // 2
    cuts = [pivots * i // len(sweeps) for i in range(len(sweeps) + 1)] if sweeps else []
    step = 0
    pass_on(0)
    next_hop = 1
    for t in range(hops):
        for s in order:
            for way in (0, 1):
                if t < arm(s, way):
                    send(way, t, s)
            if step >= gap * next_hop and next_hop < hops:
                pass_on(next_hop)
                next_hop += 1
            if step == done:
                while next_hop < hops:
                    pass_on(next_hop)
                    next_hop += 1
                gram_done()
            if step in sweeps:
                i = sweeps.index(step)
                sweep(cuts[i], cuts[i + 1])
            step += 1
    if not sweeps:
        sweep(0, pivots)

    outgoing = {}
    norms = None
    for s in order:
        sp = span(s)
        total = part[me_z, sp, :]
        for way in (0, 1):
            last = arm(s, way) - 1
            rs[way, last, s].wait_recv()
            total = total + recv[way, last, sp, :]
        if s == pairs - 1:
            norms = total[LANES:]
        up, down = total[:HALF], total[HALF:LANES]
        norm = norms[s:s + 1, :]
        for f, packed, row in (
            (2 * s, jnp.where(low, up, swap(down)), norm),
            (2 * s + 1, jnp.where(low, swap(up), down), swap(norm)),
        ):
            xsend[f, :HALF, :] = packed
            xsend[f, HALF:, :] = jnp.broadcast_to(row, (EXTRA, LANES))
            c = remote(xsend.at[f], xrecv.at[me_r], xx_s.at[f], xx_r.at[me_r], {"row": f})
            outgoing[f] = c

            @pl.when(me_r != f)
            def _(c=c):
                c.start()

            @pl.when(me_r == f)
            def _(f=f):
                xrecv[f] = xsend[f]

    for q in range(nr):
        @pl.when(me_r != q)
        def _(q=q):
            remote(xsend.at[q], xrecv.at[q], xx_s.at[q], xx_r.at[q], {"row": q}).wait_recv()

    proj, norm = [], []
    for m in range(blocks):
        a, b = xrecv[2 * m], xrecv[2 * m + 1]
        proj.append(jnp.concatenate([
            jnp.where(low, a[:HALF], swap(b[:HALF])),
            jnp.where(low, swap(a[:HALF]), b[:HALF]),
        ], axis=0) * (1.0 / 8.0))
        norm.append(jnp.where(low, a[HALF:HALF + 1], swap(b[HALF:HALF + 1])))
    proj = jnp.concatenate(proj, axis=1)
    norm = jnp.concatenate(norm, axis=1)

    def solve():
        inverse = -mat[...]
        full = jnp.concatenate([inverse * sign_hi, swap(inverse)], axis=0)
        return jnp.dot(full, proj, precision=lax.Precision.HIGHEST, preferred_element_type=F32)

    z = solve()
    inner = jnp.sum(proj * z, axis=0, keepdims=True)
    energy = jnp.sum(z * z, axis=0, keepdims=True)
    load_one = found["load"]
    first_quad = (norm - inner) / load_one
    quad_two = (first_quad - energy) / load_one
    gains = first_quad * first_quad / (quad_two * norm)
    mine = jnp.sum(gains, axis=1, keepdims=True)

    gain[me_z] = jnp.broadcast_to(mine, (1, LANES))
    copies = []
    for o in range(1, nz):
        c = remote(gain.at[me_z], gain.at[me_z], qz_s.at[o], qz_r.at[o], {"col": ahead(me_z, o, nz)})
        c.start()
        copies.append(c)
    for c in copies:
        c.wait_recv()
    pending.extend(copies)
    whole = gain[0]
    for i in range(1, nz):
        whole = whole + gain[i]
    mean_gain = whole / (HALF * nz * nr)
    ratio = GAIN_TARGET / mean_gain[:, :1]
    load_two = load_one * (1.0 + ratio * ratio)
    set_system(load_two)
    sweep(0, pivots)

    z = solve()
    quad_next = (norm - jnp.sum(proj * z, axis=0, keepdims=True)) / load_two
    final = jnp.where(it_ref[me_r] >= 2, quad_next, first_quad)
    log_power = jnp.log(norm / (final * found["power"]))
    for m in range(blocks):
        block = log_power[:, m * LANES:(m + 1) * LANES]
        lsend[2 * m] = block
        lsend[2 * m + 1] = swap(block)

    lrecv[me_f, me_r] = lsend[me_r]
    copies = []
    for of in range(nf):
        for o in range(nr):
            if of or o:
                to_f, to_r = ahead(me_f, of, nf), ahead(me_r, o, nr)
                c = remote(lsend.at[to_r], lrecv.at[me_f, me_r], ll_s.at[of, o], ll_r.at[of, o], {"freq": to_f, "row": to_r})
                c.start()
                copies.append(c)
    for c in copies:
        c.wait_recv()
    pending.extend(copies)
    band = jnp.zeros((1, LANES), F32)
    for f in range(nf):
        for r in range(nr):
            band = band + lrecv[f, r]
    for r in range(nr):
        out_ref[r:r + 1, :] = lrecv[me_f, r]
    out_ref[nr:, :] = jnp.broadcast_to(band / (freqs * nf), (EXTRA, LANES))

    for c in pending:
        c.wait_send()
    for f in range(freqs):
        @pl.when(me_r != f)
        def _(f=f):
            outgoing[f].wait_send()


def split_result(both_ref, logp_ref, band_ref):
    rows = logp_ref.shape[0]
    logp_ref[...] = both_ref[:rows, :HALF]
    band_ref[...] = both_ref[rows:rows + 1, :HALF]


def solution(mesh):
    nf, nr, nz = mesh.shape["freq"], mesh.shape["row"], mesh.shape["col"]
    pairs, hops = nr // 2, nz // 2
    rows = pairs * LANES + EXTRA
    dma = pltpu.SemaphoreType.DMA

    def body(snapshots, replicas, level_index, loading_iters):
        freqs, sensors, cands = snapshots.shape[0], snapshots.shape[1], replicas.shape[3]
        vmem = pl.BlockSpec(memory_space=pltpu.VMEM)
        smem = pl.BlockSpec(memory_space=pltpu.SMEM)
        both = pl.pallas_call(
            functools.partial(kernel, nf, nr, nz),
            out_shape=jax.ShapeDtypeStruct((freqs + EXTRA, LANES), F32),
            in_specs=[smem, smem, vmem, pl.BlockSpec(memory_space=pl.ANY)],
            out_specs=vmem,
            scratch_shapes=[
                pltpu.VMEM((freqs, 2 * sensors, cands), jnp.bfloat16),
                pltpu.VMEM((nz, rows, LANES), F32),
                pltpu.VMEM((2, hops, rows, LANES), F32),
                pltpu.VMEM((nz, sensors, LANES), jnp.bfloat16),
                pltpu.VMEM((HALF, LANES), F32),
                pltpu.VMEM((HALF, LANES), F32),
                pltpu.VMEM((nr, HALF + EXTRA, LANES), F32),
                pltpu.VMEM((nr, HALF + EXTRA, LANES), F32),
                pltpu.VMEM((nz, 1, LANES), F32),
                pltpu.VMEM((nr, 1, LANES), F32),
                pltpu.VMEM((nf, nr, 1, LANES), F32),
                dma((pairs,)),
                dma((2, hops, pairs)), dma((2, hops, pairs)),
                dma((2, hops)), dma((2, hops)),
                dma((nr,)), dma((nr,)),
                dma((nz,)), dma((nz,)),
                dma((nf, nr)), dma((nf, nr)),
            ],
            compiler_params=pltpu.CompilerParams(collective_id=0, has_side_effects=True),
            name="mvdr",
        )(level_index, loading_iters, snapshots, replicas.reshape(freqs, 2 * sensors, cands))
        log_power, band = pl.pallas_call(
            split_result,
            out_shape=(
                jax.ShapeDtypeStruct((freqs, HALF), F32),
                jax.ShapeDtypeStruct((1, HALF), F32),
            ),
            in_specs=[vmem],
            out_specs=(vmem, vmem),
            name="split",
        )(both)
        return log_power, band.reshape(HALF)

    return jax.shard_map(
        body,
        mesh=mesh,
        in_specs=(P("freq", "col", None), P("freq", None, "col", "row"), P("freq"), P("freq")),
        out_specs=(P("freq", ("row", "col")), P(("row", "col"))),
        check_vma=False,
    )
```

```python
import functools

import jax
import jax.numpy as jnp
from jax import lax
from jax.experimental import pallas as pl
from jax.experimental.pallas import tpu as pltpu
from jax.sharding import PartitionSpec as P

SENSORS = 1024
SNAPS = 64
LEVELS = 8
LANES = 128
HALF = 64
EXTRA = 8
WORDS = 88
THIRD = 40
FIELD = 21
TOP = 1048575.0
GAIN_TARGET = 0.5
MESH_ID = pl.DeviceIdType.MESH
F32 = jnp.float32


def kernel(
    nf, nr, nz,
    lvl_hbm, it_hbm, snaps_hbm, reps_hbm,
    out_ref,
    lvl_ref, it_ref, snaps_ref, reps, part, part_n, first_w, first_n, recv_w, recv_n,
    gather, mat, gram, xsend, xrecv, gain, lsend, lrecv,
    in_sem, rs_s, rs_r, rn_s, rn_r, ga_s, ga_r, xx_s, xx_r, qz_s, qz_r, ll_s, ll_r,
):
    freqs = nr
    pairs = freqs // 2
    blocks = nr // 2
    hops = nz // 2
    me_f, me_r, me_z = lax.axis_index("freq"), lax.axis_index("row"), lax.axis_index("col")
    lane = lax.broadcasted_iota(jnp.int32, (1, LANES), 1)
    low = lane < HALF
    sign_hi = jnp.where(low, 1.0, -1.0).astype(F32)
    sign_lo = jnp.where(low, -1.0, 1.0).astype(F32)
    eye = lax.broadcasted_iota(jnp.int32, (HALF, LANES), 0) == lax.broadcasted_iota(jnp.int32, (HALF, LANES), 1)

    def swap(v):
        return pltpu.roll(v, HALF, 1)

    def ahead(me, step, count):
        return lax.rem(me + (step + count), count)

    def remote(src, dst, send, got, peer):
        return pltpu.make_async_remote_copy(
            src_ref=src, dst_ref=dst, send_sem=send, recv_sem=got, device_id=peer, device_id_type=MESH_ID,
        )

    barrier = pltpu.get_barrier_semaphore()
    greet = [("col", ahead(me_z, 1, nz)), ("col", ahead(me_z, -1, nz))]
    greet += [("row", ahead(me_r, o, nr)) for o in range(1, nr)]
    greet += [("freq", ahead(me_f, o, nf)) for o in range(1, nf)]
    for axis, peer in greet:
        pl.semaphore_signal(barrier, inc=1, device_id={axis: peer}, device_id_type=MESH_ID)

    small = []
    for i, (src, dst) in enumerate(((snaps_hbm, snaps_ref), (lvl_hbm, lvl_ref), (it_hbm, it_ref))):
        c = pltpu.make_async_copy(src, dst, in_sem.at[pairs + i])
        c.start()
        small.append(c)
    fetch = []
    for s in range(pairs):
        c = pltpu.make_async_copy(reps_hbm.at[pl.ds(2 * s, 2)], reps.at[pl.ds(2 * s, 2)], in_sem.at[s])
        c.start()
        fetch.append(c)

    for c in small:
        c.wait()

    for s in range(pairs):
        fetch[s].wait()
        prods, norms = [], []
        for f in (2 * s, 2 * s + 1):
            snap = snaps_ref[f].astype(F32)
            stacked = jnp.concatenate([snap * sign_hi, swap(snap)], axis=0)
            cols = reps[f]
            prods.append(jnp.dot(stacked.T.astype(jnp.bfloat16), cols, preferred_element_type=F32))
            wide = cols.astype(F32)
            norms.append(jnp.sum(wide * wide, axis=0, keepdims=True))
        for m in range(nz // 2):
            at = slice(m * LANES, (m + 1) * LANES)
            for pair, ref in ((prods, part), (norms, part_n)):
                a, b = pair[0][:, at], pair[1][:, at]
                ref[2 * m, s] = jnp.where(low, a, swap(b))
                ref[2 * m + 1, s] = jnp.where(low, swap(a), b)
    gather[me_z] = snaps_ref[me_r]

    pl.semaphore_wait(barrier, len(greet))
    pending = []

    ring = {}

    def pass_on(h):
        for way, sign, reach in ((0, 1, hops), (1, -1, hops - 1)):
            if h < reach:
                slot = ahead(me_z, -sign * h, nz)
                if h == 0:
                    src = snaps_ref.at[me_r]
                else:
                    ring[way, h - 1].wait_recv()
                    src = gather.at[slot]
                c = remote(src, gather.at[slot], ga_s.at[way, h], ga_r.at[way, h], {"col": ahead(me_z, sign, nz)})
                c.start()
                ring[way, h] = c
                pending.append(c)

    found = {}

    def gram_done():
        ring[0, hops - 1].wait_recv()
        if hops > 1:
            ring[1, hops - 2].wait_recv()
        x = gather[...].reshape(nz * HALF, LANES)
        w = lax.dot_general(x, x, (((0,), (0,)), ((), ())), preferred_element_type=F32)
        gram[...] = (w[:HALF, :] + swap(w[HALF:, :]) * sign_hi) * (1.0 / SNAPS)
        diag = jnp.sum(jnp.where(eye, gram[...], 0.0), axis=0, keepdims=True)
        power = 2.0 * jnp.sum(diag, axis=1, keepdims=True) / (2.0 * SENSORS)
        level = lvl_ref[me_r]
        chosen = jnp.float32(0.0)
        for n in range(LEVELS):
            chosen = jnp.where(level == n, jnp.float32(2.0 ** (n / 2.0)), chosen)
        found["power"] = power
        found["load"] = chosen * power
        set_system(found["load"])

    def set_system(load):
        mat[...] = gram[...] + jnp.where(eye, load, 0.0)

    def sweep(first, last):
        def at(v, where):
            return jnp.sum(jnp.where(where, v, 0.0), axis=1, keepdims=True)

        def one(i, carry):
            k = 2 * i
            re0, re1 = lane == k, lane == k + 1
            im0, im1 = lane == k + HALF, lane == k + (HALF + 1)
            pivots = re0 | re1 | im0 | im1
            tile = mat[...]
            row0, row1 = mat[pl.ds(k, 1), :], mat[pl.ds(k + 1, 1), :]
            c0r, c0i, c1r, c1i = at(tile, re0), at(tile, im0), at(tile, re1), at(tile, im1)
            a, br, bi, c = at(row0, re0), at(row0, re1), at(row0, im1), at(row1, re1)
            r0 = jnp.where(re0, -1.0, jnp.where(pivots, 0.0, row0))
            r1 = jnp.where(re1, -1.0, jnp.where(pivots, 0.0, row1))
            j0, j1 = swap(r0) * sign_lo, swap(r1) * sign_lo
            inv = 1.0 / (a * c - (br * br + bi * bi))
            ca, cc, cr, ci = a * inv, c * inv, br * inv, bi * inv
            u0 = cc * r0 - (cr * r1 + ci * j1)
            u1 = ca * r1 - (cr * r0 - ci * j0)
            w0 = cc * j0 - (cr * j1 - ci * r1)
            w1 = ca * j1 - (cr * j0 + ci * r0)
            tile = jnp.where(pivots, 0.0, tile)
            mat[...] = tile - (c0r * u0 + c0i * w0) - (c1r * u1 + c1i * w1)
            mat[pl.ds(k, 1), :] = u0
            mat[pl.ds(k + 1, 1), :] = u1
            return carry

        lax.fori_loop(first, last, one, 0)

    def arm(s, way):
        return hops if (s < (pairs + 1) // 2) == (way == 0) else hops - 1

    def encode(v, ref):
        most = jnp.maximum(jnp.max(jnp.abs(v), axis=0, keepdims=True), 1e-30)
        q = jnp.round(v * (TOP / most)).astype(jnp.int32)
        mask = (1 << FIELD) - 1
        q_a, q_b, q_c = q[:LANES - 2 * THIRD], q[LANES - 2 * THIRD:WORDS], q[WORDS:]
        ref[:THIRD, :] = (q_a[:THIRD] & mask) | (q_c << FIELD)
        ref[THIRD:LANES - 2 * THIRD, :] = q_a[THIRD:] & mask
        ref[LANES - 2 * THIRD:, :] = (q_b & mask) | ((q_c >> (32 - FIELD)) << FIELD)
        return most * (1.0 / TOP)

    def decode(ref, unit):
        w = ref[...]
        w_a, w_b = w[:LANES - 2 * THIRD], w[LANES - 2 * THIRD:]
        q_c = ((w_b >> FIELD) << (32 - FIELD)) | lax.shift_right_logical(w_a[:THIRD], jnp.full((THIRD, LANES), FIELD, jnp.int32))
        q = jnp.concatenate([(w << (32 - FIELD)) >> (32 - FIELD), q_c], axis=0)
        return q.astype(F32) * unit

    rs = {}

    def arrived(way, t, s):
        for c in rs[way, t, s]:
            c.wait_recv()
        n = recv_n[way, t, s]
        return decode(recv_w.at[way, t, s], n[:1]), n[1:]

    def send(way, t, s):
        sign = 1 if way == 0 else -1
        dest = ahead(me_z, sign * (arm(s, way) - t), nz)
        value, norm = part[dest, s], part_n[dest, s]
        if t == 0:
            words, norms = first_w.at[way, s], first_n.at[way, s]
        else:
            more, more_n = arrived(way, t - 1, s)
            value, norm = value + more, norm + more_n
            words, norms = recv_w.at[way, t - 1, s], recv_n.at[way, t - 1, s]
        norms[:1, :] = encode(value, words)
        norms[1:, :] = norm
        to = {"col": ahead(me_z, sign, nz)}
        rs[way, t, s] = (
            remote(words, recv_w.at[way, t, s], rs_s.at[way, t, s], rs_r.at[way, t, s], to),
            remote(norms, recv_n.at[way, t, s], rn_s.at[way, t, s], rn_r.at[way, t, s], to),
        )
        for c in rs[way, t, s]:
            c.start()
            pending.append(c)

    total_steps = hops * pairs
    gap = 2 if total_steps >= 4 * hops else 1
    done = min(gap * hops + 1, total_steps - 1)
    sweeps = list(range(done + 1, total_steps - 1))
    pivots = HALF // 2
    cuts = [pivots * i // len(sweeps) for i in range(len(sweeps) + 1)] if sweeps else []
    step = 0
    pass_on(0)
    next_hop = 1
    for t in range(hops):
        for s in range(pairs):
            for way in (0, 1):
                if t < arm(s, way):
                    send(way, t, s)
            if step >= gap * next_hop and next_hop < hops:
                pass_on(next_hop)
                next_hop += 1
            if step == done:
                while next_hop < hops:
                    pass_on(next_hop)
                    next_hop += 1
                gram_done()
            if step in sweeps:
                i = sweeps.index(step)
                sweep(cuts[i], cuts[i + 1])
            step += 1
    if not sweeps:
        sweep(0, pivots)

    outgoing = {}
    for s in range(pairs):
        total, norm = part[me_z, s], part_n[me_z, s]
        for way in (0, 1):
            more, more_n = arrived(way, arm(s, way) - 1, s)
            total, norm = total + more, norm + more_n
        up, down = total[:HALF], total[HALF:]
        for f, packed, row in (
            (2 * s, jnp.where(low, up, swap(down)), norm),
            (2 * s + 1, jnp.where(low, swap(up), down), swap(norm)),
        ):
            xsend[f, :HALF, :] = packed
            xsend[f, HALF:, :] = jnp.broadcast_to(row, (EXTRA, LANES))
            c = remote(xsend.at[f], xrecv.at[me_r], xx_s.at[f], xx_r.at[me_r], {"row": f})
            outgoing[f] = c

            @pl.when(me_r != f)
            def _(c=c):
                c.start()

            @pl.when(me_r == f)
            def _(f=f):
                xrecv[f] = xsend[f]

    for q in range(nr):
        @pl.when(me_r != q)
        def _(q=q):
            remote(xsend.at[q], xrecv.at[q], xx_s.at[q], xx_r.at[q], {"row": q}).wait_recv()

    proj, norm = [], []
    for m in range(blocks):
        a, b = xrecv[2 * m], xrecv[2 * m + 1]
        proj.append(jnp.concatenate([
            jnp.where(low, a[:HALF], swap(b[:HALF])),
            jnp.where(low, swap(a[:HALF]), b[:HALF]),
        ], axis=0) * (1.0 / 8.0))
        norm.append(jnp.where(low, a[HALF:HALF + 1], swap(b[HALF:HALF + 1])))
    proj = jnp.concatenate(proj, axis=1)
    norm = jnp.concatenate(norm, axis=1)

    def solve():
        inverse = -mat[...]
        full = jnp.concatenate([inverse * sign_hi, swap(inverse)], axis=0)
        return jnp.dot(full, proj, precision=lax.Precision.HIGHEST, preferred_element_type=F32)

    z = solve()
    inner = jnp.sum(proj * z, axis=0, keepdims=True)
    energy = jnp.sum(z * z, axis=0, keepdims=True)
    load_one = found["load"]
    first_quad = (norm - inner) / load_one
    quad_two = (first_quad - energy) / load_one
    gains = first_quad * first_quad / (quad_two * norm)
    mine = jnp.sum(gains, axis=1, keepdims=True)

    gain[me_z] = jnp.broadcast_to(mine, (1, LANES))
    copies = []
    for o in range(1, nz):
        c = remote(gain.at[me_z], gain.at[me_z], qz_s.at[o], qz_r.at[o], {"col": ahead(me_z, o, nz)})
        c.start()
        copies.append(c)
    for c in copies:
        c.wait_recv()
    pending.extend(copies)
    whole = gain[0]
    for i in range(1, nz):
        whole = whole + gain[i]
    mean_gain = whole / (HALF * nz * nr)
    ratio = GAIN_TARGET / mean_gain[:, :1]
    load_two = load_one * (1.0 + ratio * ratio)
    set_system(load_two)
    sweep(0, pivots)

    z = solve()
    quad_next = (norm - jnp.sum(proj * z, axis=0, keepdims=True)) / load_two
    final = jnp.where(it_ref[me_r] >= 2, quad_next, first_quad)
    log_power = jnp.log(norm / (final * found["power"]))
    for m in range(blocks):
        block = log_power[:, m * LANES:(m + 1) * LANES]
        lsend[2 * m] = block
        lsend[2 * m + 1] = swap(block)

    lrecv[me_f, me_r] = lsend[me_r]
    copies = []
    for of in range(nf):
        for o in range(nr):
            if of or o:
                to_f, to_r = ahead(me_f, of, nf), ahead(me_r, o, nr)
                c = remote(lsend.at[to_r], lrecv.at[me_f, me_r], ll_s.at[of, o], ll_r.at[of, o], {"freq": to_f, "row": to_r})
                c.start()
                copies.append(c)
    for c in copies:
        c.wait_recv()
    pending.extend(copies)
    band = jnp.zeros((1, LANES), F32)
    for f in range(nf):
        for r in range(nr):
            band = band + lrecv[f, r]
    for r in range(nr):
        out_ref[r:r + 1, :] = lrecv[me_f, r]
    out_ref[nr:, :] = jnp.broadcast_to(band / (freqs * nf), (EXTRA, LANES))

    for c in pending:
        c.wait_send()
    for f in range(freqs):
        @pl.when(me_r != f)
        def _(f=f):
            outgoing[f].wait_send()


def split_result(both_ref, logp_ref, band_ref):
    rows = logp_ref.shape[0]
    logp_ref[...] = both_ref[:rows, :HALF]
    band_ref[...] = both_ref[rows:rows + 1, :HALF]


def solution(mesh):
    nf, nr, nz = mesh.shape["freq"], mesh.shape["row"], mesh.shape["col"]
    pairs, hops = nr // 2, nz // 2
    dma = pltpu.SemaphoreType.DMA

    def body(snapshots, replicas, level_index, loading_iters):
        freqs, sensors, cands = snapshots.shape[0], snapshots.shape[1], replicas.shape[3]
        vmem = pl.BlockSpec(memory_space=pltpu.VMEM)
        both = pl.pallas_call(
            functools.partial(kernel, nf, nr, nz),
            out_shape=jax.ShapeDtypeStruct((freqs + EXTRA, LANES), F32),
            in_specs=[pl.BlockSpec(memory_space=pl.ANY)] * 4,
            out_specs=vmem,
            scratch_shapes=[
                pltpu.SMEM((freqs,), jnp.int32),
                pltpu.SMEM((freqs,), jnp.int32),
                pltpu.VMEM((freqs, sensors, LANES), jnp.bfloat16),
                pltpu.VMEM((freqs, 2 * sensors, cands), jnp.bfloat16),
                pltpu.VMEM((nz, pairs, LANES, LANES), F32),
                pltpu.VMEM((nz, pairs, 1, LANES), F32),
                pltpu.VMEM((2, pairs, WORDS, LANES), jnp.int32),
                pltpu.VMEM((2, pairs, 2, LANES), F32),
                pltpu.VMEM((2, hops, pairs, WORDS, LANES), jnp.int32),
                pltpu.VMEM((2, hops, pairs, 2, LANES), F32),
                pltpu.VMEM((nz, sensors, LANES), jnp.bfloat16),
                pltpu.VMEM((HALF, LANES), F32),
                pltpu.VMEM((HALF, LANES), F32),
                pltpu.VMEM((nr, HALF + EXTRA, LANES), F32),
                pltpu.VMEM((nr, HALF + EXTRA, LANES), F32),
                pltpu.VMEM((nz, 1, LANES), F32),
                pltpu.VMEM((nr, 1, LANES), F32),
                pltpu.VMEM((nf, nr, 1, LANES), F32),
                dma((pairs + 3,)),
                dma((2, hops, pairs)), dma((2, hops, pairs)),
                dma((2, hops, pairs)), dma((2, hops, pairs)),
                dma((2, hops)), dma((2, hops)),
                dma((nr,)), dma((nr,)),
                dma((nz,)), dma((nz,)),
                dma((nf, nr)), dma((nf, nr)),
            ],
            compiler_params=pltpu.CompilerParams(collective_id=0, has_side_effects=True),
            name="mvdr",
        )(level_index, loading_iters, snapshots, replicas.reshape(freqs, 2 * sensors, cands))
        log_power, band = pl.pallas_call(
            split_result,
            out_shape=(
                jax.ShapeDtypeStruct((freqs, HALF), F32),
                jax.ShapeDtypeStruct((1, HALF), F32),
            ),
            in_specs=[vmem],
            out_specs=(vmem, vmem),
            name="split",
        )(both)
        return log_power, band.reshape(HALF)

    return jax.shard_map(
        body,
        mesh=mesh,
        in_specs=(P("freq", "col", None), P("freq", None, "col", "row"), P("freq"), P("freq")),
        out_specs=(P("freq", ("row", "col")), P(("row", "col"))),
        check_vma=False,
    )
```

```python
import functools

import jax
import jax.numpy as jnp
from jax import lax
from jax.experimental import pallas as pl
from jax.experimental.pallas import tpu as pltpu
from jax.sharding import PartitionSpec as P

SENSORS = 1024
SNAPS = 64
LEVELS = 8
LANES = 128
HALF = 64
EXTRA = 8
WORDS = 88
THIRD = 40
FIELD = 21
TOP = 1048575.0
GAIN_TARGET = 0.5
MESH_ID = pl.DeviceIdType.MESH
F32 = jnp.float32


def kernel(
    nf, nr, nz,
    lvl_hbm, it_hbm, snaps_hbm, reps_hbm,
    out_ref,
    lvl_ref, it_ref, snaps_ref, reps, part, part_n, first_w, first_n, recv_w, recv_n,
    gather, mat, gram, xsend, xrecv, gain, lsend, lrecv,
    in_sem, rs_s, rs_r, rn_s, rn_r, ga_s, ga_r, xx_s, xx_r, qz_s, qz_r, ll_s, ll_r,
):
    freqs = nr
    pairs = freqs // 2
    blocks = nr // 2
    hops = nz // 2
    me_f, me_r, me_z = lax.axis_index("freq"), lax.axis_index("row"), lax.axis_index("col")
    lane = lax.broadcasted_iota(jnp.int32, (1, LANES), 1)
    low = lane < HALF
    sign_hi = jnp.where(low, 1.0, -1.0).astype(F32)
    sign_lo = jnp.where(low, -1.0, 1.0).astype(F32)
    eye = lax.broadcasted_iota(jnp.int32, (HALF, LANES), 0) == lax.broadcasted_iota(jnp.int32, (HALF, LANES), 1)

    def swap(v):
        return pltpu.roll(v, HALF, 1)

    def ahead(me, step, count):
        return lax.rem(me + (step + count), count)

    def remote(src, dst, send, got, peer):
        return pltpu.make_async_remote_copy(
            src_ref=src, dst_ref=dst, send_sem=send, recv_sem=got, device_id=peer, device_id_type=MESH_ID,
        )

    barrier = pltpu.get_barrier_semaphore()
    greet = [("col", ahead(me_z, 1, nz)), ("col", ahead(me_z, -1, nz))]
    greet += [("row", ahead(me_r, o, nr)) for o in range(1, nr)]
    greet += [("freq", ahead(me_f, o, nf)) for o in range(1, nf)]
    for axis, peer in greet:
        pl.semaphore_signal(barrier, inc=1, device_id={axis: peer}, device_id_type=MESH_ID)

    small = []
    for i, (src, dst) in enumerate(((snaps_hbm, snaps_ref), (lvl_hbm, lvl_ref), (it_hbm, it_ref))):
        c = pltpu.make_async_copy(src, dst, in_sem.at[freqs + i])
        c.start()
        small.append(c)
    fetch = []
    for f in range(freqs):
        c = pltpu.make_async_copy(reps_hbm.at[f], reps.at[f], in_sem.at[f])
        c.start()
        fetch.append(c)

    for c in small:
        c.wait()

    for s in range(pairs):
        prods, norms = [], []
        for f in (s, s + pairs):
            fetch[f].wait()
            snap = snaps_ref[f].astype(F32)
            stacked = jnp.concatenate([snap * sign_hi, swap(snap)], axis=0)
            cols = reps[f]
            prods.append(jnp.dot(stacked.T.astype(jnp.bfloat16), cols, preferred_element_type=F32))
            wide = cols.astype(F32)
            norms.append(jnp.sum(wide * wide, axis=0, keepdims=True))
        for m in range(nz // 2):
            at = slice(m * LANES, (m + 1) * LANES)
            for pair, ref in ((prods, part), (norms, part_n)):
                a, b = pair[0][:, at], pair[1][:, at]
                ref[2 * m, s] = jnp.where(low, a, swap(b))
                ref[2 * m + 1, s] = jnp.where(low, swap(a), b)
    gather[me_z] = snaps_ref[me_r]

    pl.semaphore_wait(barrier, len(greet))
    pending = []

    ring = {}

    def pass_on(h):
        for way, sign, reach in ((0, 1, hops), (1, -1, hops - 1)):
            if h < reach:
                slot = ahead(me_z, -sign * h, nz)
                if h == 0:
                    src = snaps_ref.at[me_r]
                else:
                    ring[way, h - 1].wait_recv()
                    src = gather.at[slot]
                c = remote(src, gather.at[slot], ga_s.at[way, h], ga_r.at[way, h], {"col": ahead(me_z, sign, nz)})
                c.start()
                ring[way, h] = c
                pending.append(c)

    found = {}

    def gram_done():
        ring[0, hops - 1].wait_recv()
        if hops > 1:
            ring[1, hops - 2].wait_recv()
        x = gather[...].reshape(nz * HALF, LANES)
        w = lax.dot_general(x, x, (((0,), (0,)), ((), ())), preferred_element_type=F32)
        gram[...] = (w[:HALF, :] + swap(w[HALF:, :]) * sign_hi) * (1.0 / SNAPS)
        diag = jnp.sum(jnp.where(eye, gram[...], 0.0), axis=0, keepdims=True)
        power = 2.0 * jnp.sum(diag, axis=1, keepdims=True) / (2.0 * SENSORS)
        level = lvl_ref[me_r]
        chosen = jnp.float32(0.0)
        for n in range(LEVELS):
            chosen = jnp.where(level == n, jnp.float32(2.0 ** (n / 2.0)), chosen)
        found["power"] = power
        found["load"] = chosen * power
        set_system(found["load"])

    def set_system(load):
        mat[...] = gram[...] + jnp.where(eye, load, 0.0)

    def sweep(first, last):
        def at(v, where):
            return jnp.sum(jnp.where(where, v, 0.0), axis=1, keepdims=True)

        def one(i, carry):
            k = 2 * i
            re0, re1 = lane == k, lane == k + 1
            im0, im1 = lane == k + HALF, lane == k + (HALF + 1)
            pivots = re0 | re1 | im0 | im1
            tile = mat[...]
            row0, row1 = mat[pl.ds(k, 1), :], mat[pl.ds(k + 1, 1), :]
            c0r, c0i, c1r, c1i = at(tile, re0), at(tile, im0), at(tile, re1), at(tile, im1)
            a, br, bi, c = at(row0, re0), at(row0, re1), at(row0, im1), at(row1, re1)
            r0 = jnp.where(re0, -1.0, jnp.where(pivots, 0.0, row0))
            r1 = jnp.where(re1, -1.0, jnp.where(pivots, 0.0, row1))
            j0, j1 = swap(r0) * sign_lo, swap(r1) * sign_lo
            inv = 1.0 / (a * c - (br * br + bi * bi))
            ca, cc, cr, ci = a * inv, c * inv, br * inv, bi * inv
            u0 = cc * r0 - (cr * r1 + ci * j1)
            u1 = ca * r1 - (cr * r0 - ci * j0)
            w0 = cc * j0 - (cr * j1 - ci * r1)
            w1 = ca * j1 - (cr * j0 + ci * r0)
            tile = jnp.where(pivots, 0.0, tile)
            mat[...] = tile - (c0r * u0 + c0i * w0) - (c1r * u1 + c1i * w1)
            mat[pl.ds(k, 1), :] = u0
            mat[pl.ds(k + 1, 1), :] = u1
            return carry

        lax.fori_loop(first, last, one, 0)

    def arm(s, way):
        return hops if (s < (pairs + 1) // 2) == (way == 0) else hops - 1

    def encode(v, ref):
        most = jnp.maximum(jnp.max(jnp.abs(v), axis=0, keepdims=True), 1e-30)
        q = jnp.round(v * (TOP / most)).astype(jnp.int32)
        mask = (1 << FIELD) - 1
        q_a, q_b, q_c = q[:LANES - 2 * THIRD], q[LANES - 2 * THIRD:WORDS], q[WORDS:]
        ref[:THIRD, :] = (q_a[:THIRD] & mask) | (q_c << FIELD)
        ref[THIRD:LANES - 2 * THIRD, :] = q_a[THIRD:] & mask
        ref[LANES - 2 * THIRD:, :] = (q_b & mask) | ((q_c >> (32 - FIELD)) << FIELD)
        return most * (1.0 / TOP)

    def decode(ref, unit):
        w = ref[...]
        w_a, w_b = w[:LANES - 2 * THIRD], w[LANES - 2 * THIRD:]
        q_c = ((w_b >> FIELD) << (32 - FIELD)) | lax.shift_right_logical(w_a[:THIRD], jnp.full((THIRD, LANES), FIELD, jnp.int32))
        q = jnp.concatenate([(w << (32 - FIELD)) >> (32 - FIELD), q_c], axis=0)
        return q.astype(F32) * unit

    rs = {}

    def arrived(way, t, s):
        for c in rs[way, t, s]:
            c.wait_recv()
        n = recv_n[way, t, s]
        return decode(recv_w.at[way, t, s], n[:1]), n[1:]

    def send(way, t, s):
        sign = 1 if way == 0 else -1
        dest = ahead(me_z, sign * (arm(s, way) - t), nz)
        value, norm = part[dest, s], part_n[dest, s]
        if t == 0:
            words, norms = first_w.at[way, s], first_n.at[way, s]
        else:
            more, more_n = arrived(way, t - 1, s)
            value, norm = value + more, norm + more_n
            words, norms = recv_w.at[way, t - 1, s], recv_n.at[way, t - 1, s]
        norms[:1, :] = encode(value, words)
        norms[1:, :] = norm
        to = {"col": ahead(me_z, sign, nz)}
        rs[way, t, s] = (
            remote(words, recv_w.at[way, t, s], rs_s.at[way, t, s], rs_r.at[way, t, s], to),
            remote(norms, recv_n.at[way, t, s], rn_s.at[way, t, s], rn_r.at[way, t, s], to),
        )
        for c in rs[way, t, s]:
            c.start()
            pending.append(c)

    total_steps = hops * pairs
    gap = 3 if total_steps > 3 * hops + 4 else 1
    done = min(gap * (hops - 1) + 4, total_steps - 1)
    pivots = HALF // 2
    swept, share = 0, 3
    step = 0
    pass_on(0)
    next_hop = 1
    for t in range(hops):
        for s in range(pairs):
            if next_hop < hops and step >= gap * next_hop:
                pass_on(next_hop)
                next_hop += 1
            for way in (0, 1):
                if t < arm(s, way):
                    send(way, t, s)
            if step == done:
                while next_hop < hops:
                    pass_on(next_hop)
                    next_hop += 1
                gram_done()
            elif step > done:
                sweep(swept, swept + share)
                swept += share
            step += 1

    outgoing = {}
    for s in range(pairs):
        total, norm = part[me_z, s], part_n[me_z, s]
        for way in (0, 1):
            more, more_n = arrived(way, arm(s, way) - 1, s)
            total, norm = total + more, norm + more_n
        up, down = total[:HALF], total[HALF:]
        for f, packed, row in (
            (s, jnp.where(low, up, swap(down)), norm),
            (s + pairs, jnp.where(low, swap(up), down), swap(norm)),
        ):
            xsend[f, :HALF, :] = packed
            xsend[f, HALF:, :] = jnp.broadcast_to(row, (EXTRA, LANES))
            c = remote(xsend.at[f], xrecv.at[me_r], xx_s.at[f], xx_r.at[me_r], {"row": f})
            outgoing[f] = c

            @pl.when(me_r != f)
            def _(c=c):
                c.start()

            @pl.when(me_r == f)
            def _(f=f):
                xrecv[f] = xsend[f]

    sweep(swept, pivots)
    for q in range(nr):
        @pl.when(me_r != q)
        def _(q=q):
            remote(xsend.at[q], xrecv.at[q], xx_s.at[q], xx_r.at[q], {"row": q}).wait_recv()

    proj, norm = [], []
    for m in range(blocks):
        a, b = xrecv[2 * m], xrecv[2 * m + 1]
        proj.append(jnp.concatenate([
            jnp.where(low, a[:HALF], swap(b[:HALF])),
            jnp.where(low, swap(a[:HALF]), b[:HALF]),
        ], axis=0) * (1.0 / 8.0))
        norm.append(jnp.where(low, a[HALF:HALF + 1], swap(b[HALF:HALF + 1])))
    proj = jnp.concatenate(proj, axis=1)
    norm = jnp.concatenate(norm, axis=1)

    def solve():
        inverse = -mat[...]
        full = jnp.concatenate([inverse * sign_hi, swap(inverse)], axis=0)
        return jnp.dot(full, proj, precision=lax.Precision.HIGHEST, preferred_element_type=F32)

    z = solve()
    inner = jnp.sum(proj * z, axis=0, keepdims=True)
    energy = jnp.sum(z * z, axis=0, keepdims=True)
    load_one = found["load"]
    first_quad = (norm - inner) / load_one
    quad_two = (first_quad - energy) / load_one
    gains = first_quad * first_quad / (quad_two * norm)
    mine = jnp.sum(gains, axis=1, keepdims=True)

    gain[me_z] = jnp.broadcast_to(mine, (1, LANES))
    copies = []
    for o in range(1, nz):
        c = remote(gain.at[me_z], gain.at[me_z], qz_s.at[o], qz_r.at[o], {"col": ahead(me_z, o, nz)})
        c.start()
        copies.append(c)
    for c in copies:
        c.wait_recv()
    pending.extend(copies)
    whole = gain[0]
    for i in range(1, nz):
        whole = whole + gain[i]
    mean_gain = whole / (HALF * nz * nr)
    ratio = GAIN_TARGET / mean_gain[:, :1]
    load_two = load_one * (1.0 + ratio * ratio)
    set_system(load_two)
    sweep(0, pivots)

    z = solve()
    quad_next = (norm - jnp.sum(proj * z, axis=0, keepdims=True)) / load_two
    final = jnp.where(it_ref[me_r] >= 2, quad_next, first_quad)
    log_power = jnp.log(norm / (final * found["power"]))
    for m in range(blocks):
        block = log_power[:, m * LANES:(m + 1) * LANES]
        lsend[2 * m] = block
        lsend[2 * m + 1] = swap(block)

    lrecv[me_f, me_r] = lsend[me_r]
    copies = []
    for of in range(nf):
        for o in range(nr):
            if of or o:
                to_f, to_r = ahead(me_f, of, nf), ahead(me_r, o, nr)
                c = remote(lsend.at[to_r], lrecv.at[me_f, me_r], ll_s.at[of, o], ll_r.at[of, o], {"freq": to_f, "row": to_r})
                c.start()
                copies.append(c)
    for c in copies:
        c.wait_recv()
    pending.extend(copies)
    band = jnp.zeros((1, LANES), F32)
    for f in range(nf):
        for r in range(nr):
            band = band + lrecv[f, r]
    for r in range(nr):
        out_ref[r:r + 1, :] = lrecv[me_f, r]
    out_ref[nr:, :] = jnp.broadcast_to(band / (freqs * nf), (EXTRA, LANES))

    for c in pending:
        c.wait_send()
    for f in range(freqs):
        @pl.when(me_r != f)
        def _(f=f):
            outgoing[f].wait_send()


def split_result(both_ref, logp_ref, band_ref):
    rows = logp_ref.shape[0]
    logp_ref[...] = both_ref[:rows, :HALF]
    band_ref[...] = both_ref[rows:rows + 1, :HALF]


def solution(mesh):
    nf, nr, nz = mesh.shape["freq"], mesh.shape["row"], mesh.shape["col"]
    pairs, hops = nr // 2, nz // 2
    dma = pltpu.SemaphoreType.DMA

    def body(snapshots, replicas, level_index, loading_iters):
        freqs, sensors, cands = snapshots.shape[0], snapshots.shape[1], replicas.shape[3]
        vmem = pl.BlockSpec(memory_space=pltpu.VMEM)
        both = pl.pallas_call(
            functools.partial(kernel, nf, nr, nz),
            out_shape=jax.ShapeDtypeStruct((freqs + EXTRA, LANES), F32),
            in_specs=[pl.BlockSpec(memory_space=pl.ANY)] * 4,
            out_specs=vmem,
            scratch_shapes=[
                pltpu.SMEM((freqs,), jnp.int32),
                pltpu.SMEM((freqs,), jnp.int32),
                pltpu.VMEM((freqs, sensors, LANES), jnp.bfloat16),
                pltpu.VMEM((freqs, 2 * sensors, cands), jnp.bfloat16),
                pltpu.VMEM((nz, pairs, LANES, LANES), F32),
                pltpu.VMEM((nz, pairs, 1, LANES), F32),
                pltpu.VMEM((2, pairs, WORDS, LANES), jnp.int32),
                pltpu.VMEM((2, pairs, 2, LANES), F32),
                pltpu.VMEM((2, hops, pairs, WORDS, LANES), jnp.int32),
                pltpu.VMEM((2, hops, pairs, 2, LANES), F32),
                pltpu.VMEM((nz, sensors, LANES), jnp.bfloat16),
                pltpu.VMEM((HALF, LANES), F32),
                pltpu.VMEM((HALF, LANES), F32),
                pltpu.VMEM((nr, HALF + EXTRA, LANES), F32),
                pltpu.VMEM((nr, HALF + EXTRA, LANES), F32),
                pltpu.VMEM((nz, 1, LANES), F32),
                pltpu.VMEM((nr, 1, LANES), F32),
                pltpu.VMEM((nf, nr, 1, LANES), F32),
                dma((freqs + 3,)),
                dma((2, hops, pairs)), dma((2, hops, pairs)),
                dma((2, hops, pairs)), dma((2, hops, pairs)),
                dma((2, hops)), dma((2, hops)),
                dma((nr,)), dma((nr,)),
                dma((nz,)), dma((nz,)),
                dma((nf, nr)), dma((nf, nr)),
            ],
            compiler_params=pltpu.CompilerParams(collective_id=0, has_side_effects=True),
            name="mvdr",
        )(level_index, loading_iters, snapshots, replicas.reshape(freqs, 2 * sensors, cands))
        log_power, band = pl.pallas_call(
            split_result,
            out_shape=(
                jax.ShapeDtypeStruct((freqs, HALF), F32),
                jax.ShapeDtypeStruct((1, HALF), F32),
            ),
            in_specs=[vmem],
            out_specs=(vmem, vmem),
            name="split",
        )(both)
        return log_power, band.reshape(HALF)

    return jax.shard_map(
        body,
        mesh=mesh,
        in_specs=(P("freq", "col", None), P("freq", None, "col", "row"), P("freq"), P("freq")),
        out_specs=(P("freq", ("row", "col")), P(("row", "col"))),
        check_vma=False,
    )
```

```python
import functools

import jax
import jax.numpy as jnp
from jax import lax
from jax.experimental import pallas as pl
from jax.experimental.pallas import tpu as pltpu
from jax.sharding import PartitionSpec as P

SENSORS = 1024
SNAPS = 64
LEVELS = 8
LANES = 128
HALF = 64
EXTRA = 8
WORDS = 80
GROUP = 16
FIELD = 20
TOP = 524287.0
GAIN_TARGET = 0.5
MESH_ID = pl.DeviceIdType.MESH
F32 = jnp.float32


def kernel(
    nf, nr, nz,
    lvl_hbm, it_hbm, snaps_hbm, reps_hbm,
    out_ref,
    lvl_ref, it_ref, snaps_ref, reps, part, part_n, first_w, first_n, recv_w, recv_n,
    gather, mat, gram, xsend, xrecv, gain, lsend, lrecv,
    in_sem, rs_s, rs_r, rn_s, rn_r, ga_s, ga_r, xx_s, xx_r, qz_s, qz_r, ll_s, ll_r,
):
    freqs = nr
    pairs = freqs // 2
    blocks = nr // 2
    hops = nz // 2
    me_f, me_r, me_z = lax.axis_index("freq"), lax.axis_index("row"), lax.axis_index("col")
    lane = lax.broadcasted_iota(jnp.int32, (1, LANES), 1)
    low = lane < HALF
    sign_hi = jnp.where(low, 1.0, -1.0).astype(F32)
    sign_lo = jnp.where(low, -1.0, 1.0).astype(F32)
    eye = lax.broadcasted_iota(jnp.int32, (HALF, LANES), 0) == lax.broadcasted_iota(jnp.int32, (HALF, LANES), 1)

    def swap(v):
        return pltpu.roll(v, HALF, 1)

    def ahead(me, step, count):
        return lax.rem(me + (step + count), count)

    def remote(src, dst, send, got, peer):
        return pltpu.make_async_remote_copy(
            src_ref=src, dst_ref=dst, send_sem=send, recv_sem=got, device_id=peer, device_id_type=MESH_ID,
        )

    barrier = pltpu.get_barrier_semaphore()
    greet = [("col", ahead(me_z, 1, nz)), ("col", ahead(me_z, -1, nz))]
    greet += [("row", ahead(me_r, o, nr)) for o in range(1, nr)]
    greet += [("freq", ahead(me_f, o, nf)) for o in range(1, nf)]
    for axis, peer in greet:
        pl.semaphore_signal(barrier, inc=1, device_id={axis: peer}, device_id_type=MESH_ID)

    small = []
    for i, (src, dst) in enumerate(((snaps_hbm, snaps_ref), (lvl_hbm, lvl_ref), (it_hbm, it_ref))):
        c = pltpu.make_async_copy(src, dst, in_sem.at[freqs + i])
        c.start()
        small.append(c)
    fetch = []
    for f in range(freqs):
        c = pltpu.make_async_copy(reps_hbm.at[f], reps.at[f], in_sem.at[f])
        c.start()
        fetch.append(c)

    for c in small:
        c.wait()

    for s in range(pairs):
        prods, norms = [], []
        for f in (s, s + pairs):
            fetch[f].wait()
            snap = snaps_ref[f].astype(F32)
            stacked = jnp.concatenate([snap * sign_hi, swap(snap)], axis=0)
            cols = reps[f]
            prods.append(jnp.dot(stacked.T.astype(jnp.bfloat16), cols, preferred_element_type=F32))
            wide = cols.astype(F32)
            norms.append(jnp.sum(wide * wide, axis=0, keepdims=True))
        for m in range(nz // 2):
            at = slice(m * LANES, (m + 1) * LANES)
            for pair, ref in ((prods, part), (norms, part_n)):
                a, b = pair[0][:, at], pair[1][:, at]
                ref[2 * m, s] = jnp.where(low, a, swap(b))
                ref[2 * m + 1, s] = jnp.where(low, swap(a), b)
    gather[me_z] = snaps_ref[me_r]

    def arm(s, way):
        return hops if (s < (pairs + 1) // 2) == (way == 0) else hops - 1

    def encode(v, ref):
        most = jnp.maximum(jnp.max(jnp.abs(v), axis=0, keepdims=True), 1e-30)
        q = jnp.round(v * (TOP / most)).astype(jnp.int32) & ((1 << FIELD) - 1)
        g = [q[i * GROUP:(i + 1) * GROUP] for i in range(8)]
        g_6, g_7 = g[6], g[7]
        tops = (
            g[5],
            lax.shift_right_logical(g[5], jnp.full((GROUP, LANES), 12, jnp.int32)) | (g_6 << 8),
            g_6 >> 4,
            (g_6 >> 16) | (g_7 << 4),
            g_7 >> 8,
        )
        for i, top in enumerate(tops):
            ref[i * GROUP:(i + 1) * GROUP, :] = g[i] | (top << FIELD)
        return most * (1.0 / TOP)

    def decode(ref, unit):
        w = ref[...]
        t = lax.shift_right_logical(w, jnp.full((WORDS, LANES), FIELD, jnp.int32))
        t = [t[i * GROUP:(i + 1) * GROUP] for i in range(5)]
        high = jnp.concatenate([
            t[0] | (t[1] << 12),
            (t[1] >> 8) | (t[2] << 4) | (t[3] << 16),
            (t[3] >> 4) | (t[4] << 8),
        ], axis=0)
        q = jnp.concatenate([w, high], axis=0)
        return ((q << (32 - FIELD)) >> (32 - FIELD)).astype(F32) * unit

    def target(way, t, s):
        return ahead(me_z, (1 if way == 0 else -1) * (arm(s, way) - t), nz)

    for s in range(pairs):
        for way in (0, 1):
            dest = target(way, 0, s)
            first_n[way, s, :1, :] = encode(part[dest, s], first_w.at[way, s])
            first_n[way, s, 1:, :] = part_n[dest, s]

    pl.semaphore_wait(barrier, len(greet))
    pending = []

    ring = {}

    def pass_on(h):
        for way, sign, reach in ((0, 1, hops), (1, -1, hops - 1)):
            if h < reach:
                slot = ahead(me_z, -sign * h, nz)
                if h == 0:
                    src = snaps_ref.at[me_r]
                else:
                    ring[way, h - 1].wait_recv()
                    src = gather.at[slot]
                c = remote(src, gather.at[slot], ga_s.at[way, h], ga_r.at[way, h], {"col": ahead(me_z, sign, nz)})
                c.start()
                ring[way, h] = c
                pending.append(c)

    found = {}

    def gram_done():
        ring[0, hops - 1].wait_recv()
        if hops > 1:
            ring[1, hops - 2].wait_recv()
        x = gather[...].reshape(nz * HALF, LANES)
        w = lax.dot_general(x, x, (((0,), (0,)), ((), ())), preferred_element_type=F32)
        gram[...] = (w[:HALF, :] + swap(w[HALF:, :]) * sign_hi) * (1.0 / SNAPS)
        diag = jnp.sum(jnp.where(eye, gram[...], 0.0), axis=0, keepdims=True)
        power = 2.0 * jnp.sum(diag, axis=1, keepdims=True) / (2.0 * SENSORS)
        level = lvl_ref[me_r]
        chosen = jnp.float32(0.0)
        for n in range(LEVELS):
            chosen = jnp.where(level == n, jnp.float32(2.0 ** (n / 2.0)), chosen)
        found["power"] = power
        found["load"] = chosen * power
        set_system(found["load"])

    def set_system(load):
        mat[...] = gram[...] + jnp.where(eye, load, 0.0)

    def sweep(first, last):
        def at(v, where):
            return jnp.sum(jnp.where(where, v, 0.0), axis=1, keepdims=True)

        def one(i, carry):
            k = 2 * i
            re0, re1 = lane == k, lane == k + 1
            im0, im1 = lane == k + HALF, lane == k + (HALF + 1)
            pivots = re0 | re1 | im0 | im1
            tile = mat[...]
            row0, row1 = mat[pl.ds(k, 1), :], mat[pl.ds(k + 1, 1), :]
            a, br, bi, c = at(row0, re0), at(row0, re1), at(row0, im1), at(row1, re1)
            c0r, c0i, c1r, c1i = at(tile, re0), at(tile, im0), at(tile, re1), at(tile, im1)
            r0 = jnp.where(re0, -1.0, jnp.where(pivots, 0.0, row0))
            r1 = jnp.where(re1, -1.0, jnp.where(pivots, 0.0, row1))
            j0, j1 = swap(r0) * sign_lo, swap(r1) * sign_lo
            inv = 1.0 / (a * c - (br * br + bi * bi))
            ca, cc, cr, ci = a * inv, c * inv, br * inv, bi * inv
            u0 = cc * r0 - (cr * r1 + ci * j1)
            u1 = ca * r1 - (cr * r0 - ci * j0)
            w0 = cc * j0 - (cr * j1 - ci * r1)
            w1 = ca * j1 - (cr * j0 + ci * r0)
            tile = jnp.where(pivots, 0.0, tile)
            mat[...] = tile - (c0r * u0 + c0i * w0) - (c1r * u1 + c1i * w1)
            mat[pl.ds(k, 1), :] = u0
            mat[pl.ds(k + 1, 1), :] = u1
            return carry

        lax.fori_loop(first, last, one, 0)

    rs = {}

    def arrived(way, t, s):
        for c in rs[way, t, s]:
            c.wait_recv()
        n = recv_n[way, t, s]
        return decode(recv_w.at[way, t, s], n[:1]), n[1:]

    def send(way, t, s):
        if t == 0:
            words, norms = first_w.at[way, s], first_n.at[way, s]
        else:
            dest = target(way, t, s)
            more, more_n = arrived(way, t - 1, s)
            words, norms = recv_w.at[way, t - 1, s], recv_n.at[way, t - 1, s]
            norms[:1, :] = encode(part[dest, s] + more, words)
            norms[1:, :] = part_n[dest, s] + more_n
        to = {"col": ahead(me_z, 1 if way == 0 else -1, nz)}
        rs[way, t, s] = (
            remote(words, recv_w.at[way, t, s], rs_s.at[way, t, s], rs_r.at[way, t, s], to),
            remote(norms, recv_n.at[way, t, s], rn_s.at[way, t, s], rn_r.at[way, t, s], to),
        )
        for c in rs[way, t, s]:
            c.start()
            pending.append(c)

    half = (pairs + 1) // 2
    total_steps = hops * pairs
    gap = 3 if total_steps > 3 * hops + 4 else 1
    done = min(gap * (hops - 1) + 4, total_steps - 1)
    pivots = HALF // 2
    swept, share = 0, 3
    step = 0
    pass_on(0)
    next_hop = 1
    for t in range(hops):
        for s in range(pairs):
            if next_hop < hops and step >= gap * next_hop:
                pass_on(next_hop)
                next_hop += 1
            for way in (0, 1):
                turn = (s + way * half) % pairs
                if t < arm(turn, way):
                    send(way, t, turn)
            if step == done:
                while next_hop < hops:
                    pass_on(next_hop)
                    next_hop += 1
                gram_done()
            elif step > done:
                sweep(swept, swept + share)
                swept += share
            step += 1

    outgoing = {}
    for s in sorted(range(pairs), key=lambda s: s % half):
        total, norm = part[me_z, s], part_n[me_z, s]
        for way in (0, 1):
            more, more_n = arrived(way, arm(s, way) - 1, s)
            total, norm = total + more, norm + more_n
        up, down = total[:HALF], total[HALF:]
        for f, packed, row in (
            (s, jnp.where(low, up, swap(down)), norm),
            (s + pairs, jnp.where(low, swap(up), down), swap(norm)),
        ):
            xsend[f, :HALF, :] = packed
            xsend[f, HALF:, :] = jnp.broadcast_to(row, (EXTRA, LANES))
            c = remote(xsend.at[f], xrecv.at[me_r], xx_s.at[f], xx_r.at[me_r], {"row": f})
            outgoing[f] = c

            @pl.when(me_r != f)
            def _(c=c):
                c.start()

            @pl.when(me_r == f)
            def _(f=f):
                xrecv[f] = xsend[f]

    sweep(swept, pivots)
    for q in range(nr):
        @pl.when(me_r != q)
        def _(q=q):
            remote(xsend.at[q], xrecv.at[q], xx_s.at[q], xx_r.at[q], {"row": q}).wait_recv()

    proj, norm = [], []
    for m in range(blocks):
        a, b = xrecv[2 * m], xrecv[2 * m + 1]
        proj.append(jnp.concatenate([
            jnp.where(low, a[:HALF], swap(b[:HALF])),
            jnp.where(low, swap(a[:HALF]), b[:HALF]),
        ], axis=0) * (1.0 / 8.0))
        norm.append(jnp.where(low, a[HALF:HALF + 1], swap(b[HALF:HALF + 1])))
    proj = jnp.concatenate(proj, axis=1)
    norm = jnp.concatenate(norm, axis=1)

    def solve():
        inverse = -mat[...]
        full = jnp.concatenate([inverse * sign_hi, swap(inverse)], axis=0)
        return jnp.dot(full, proj, precision=lax.Precision.HIGHEST, preferred_element_type=F32)

    z = solve()
    inner = jnp.sum(proj * z, axis=0, keepdims=True)
    energy = jnp.sum(z * z, axis=0, keepdims=True)
    load_one = found["load"]
    first_quad = (norm - inner) / load_one
    quad_two = (first_quad - energy) / load_one
    gains = first_quad * first_quad / (quad_two * norm)
    mine = jnp.sum(gains, axis=1, keepdims=True)

    gain[me_z] = jnp.broadcast_to(mine, (1, LANES))
    copies = []
    for o in sorted(range(1, nz), key=lambda o: abs(o - hops)):
        c = remote(gain.at[me_z], gain.at[me_z], qz_s.at[o], qz_r.at[o], {"col": ahead(me_z, o, nz)})
        c.start()
        copies.append(c)
    for c in copies:
        c.wait_recv()
    pending.extend(copies)
    whole = gain[0]
    for i in range(1, nz):
        whole = whole + gain[i]
    mean_gain = whole / (HALF * nz * nr)
    ratio = GAIN_TARGET / mean_gain[:, :1]
    load_two = load_one * (1.0 + ratio * ratio)
    set_system(load_two)
    sweep(0, pivots)

    z = solve()
    quad_next = (norm - jnp.sum(proj * z, axis=0, keepdims=True)) / load_two
    final = jnp.where(it_ref[me_r] >= 2, quad_next, first_quad)
    log_power = jnp.log(norm / (final * found["power"]))
    for m in range(blocks):
        block = log_power[:, m * LANES:(m + 1) * LANES]
        lsend[2 * m] = block
        lsend[2 * m + 1] = swap(block)

    lrecv[me_f, me_r] = lsend[me_r]
    copies = []
    for of in range(nf):
        for o in range(nr):
            if of or o:
                to_f, to_r = ahead(me_f, of, nf), ahead(me_r, o, nr)
                c = remote(lsend.at[to_r], lrecv.at[me_f, me_r], ll_s.at[of, o], ll_r.at[of, o], {"freq": to_f, "row": to_r})
                c.start()
                copies.append(c)
    for c in copies:
        c.wait_recv()
    pending.extend(copies)
    band = jnp.zeros((1, LANES), F32)
    for f in range(nf):
        for r in range(nr):
            band = band + lrecv[f, r]
    for r in range(nr):
        out_ref[r:r + 1, :] = lrecv[me_f, r]
    out_ref[nr:, :] = jnp.broadcast_to(band / (freqs * nf), (EXTRA, LANES))

    for c in pending:
        c.wait_send()
    for f in range(freqs):
        @pl.when(me_r != f)
        def _(f=f):
            outgoing[f].wait_send()


def split_result(both_ref, logp_ref, band_ref):
    rows = logp_ref.shape[0]
    logp_ref[...] = both_ref[:rows, :HALF]
    band_ref[...] = both_ref[rows:rows + 1, :HALF]


def solution(mesh):
    nf, nr, nz = mesh.shape["freq"], mesh.shape["row"], mesh.shape["col"]
    pairs, hops = nr // 2, nz // 2
    dma = pltpu.SemaphoreType.DMA

    def body(snapshots, replicas, level_index, loading_iters):
        freqs, sensors, cands = snapshots.shape[0], snapshots.shape[1], replicas.shape[3]
        vmem = pl.BlockSpec(memory_space=pltpu.VMEM)
        both = pl.pallas_call(
            functools.partial(kernel, nf, nr, nz),
            out_shape=jax.ShapeDtypeStruct((freqs + EXTRA, LANES), F32),
            in_specs=[pl.BlockSpec(memory_space=pl.ANY)] * 4,
            out_specs=vmem,
            scratch_shapes=[
                pltpu.SMEM((freqs,), jnp.int32),
                pltpu.SMEM((freqs,), jnp.int32),
                pltpu.VMEM((freqs, sensors, LANES), jnp.bfloat16),
                pltpu.VMEM((freqs, 2 * sensors, cands), jnp.bfloat16),
                pltpu.VMEM((nz, pairs, LANES, LANES), F32),
                pltpu.VMEM((nz, pairs, 1, LANES), F32),
                pltpu.VMEM((2, pairs, WORDS, LANES), jnp.int32),
                pltpu.VMEM((2, pairs, 2, LANES), F32),
                pltpu.VMEM((2, hops, pairs, WORDS, LANES), jnp.int32),
                pltpu.VMEM((2, hops, pairs, 2, LANES), F32),
                pltpu.VMEM((nz, sensors, LANES), jnp.bfloat16),
                pltpu.VMEM((HALF, LANES), F32),
                pltpu.VMEM((HALF, LANES), F32),
                pltpu.VMEM((nr, HALF + EXTRA, LANES), F32),
                pltpu.VMEM((nr, HALF + EXTRA, LANES), F32),
                pltpu.VMEM((nz, 1, LANES), F32),
                pltpu.VMEM((nr, 1, LANES), F32),
                pltpu.VMEM((nf, nr, 1, LANES), F32),
                dma((freqs + 3,)),
                dma((2, hops, pairs)), dma((2, hops, pairs)),
                dma((2, hops, pairs)), dma((2, hops, pairs)),
                dma((2, hops)), dma((2, hops)),
                dma((nr,)), dma((nr,)),
                dma((nz,)), dma((nz,)),
                dma((nf, nr)), dma((nf, nr)),
            ],
            compiler_params=pltpu.CompilerParams(collective_id=0, has_side_effects=True),
            name="mvdr",
        )(level_index, loading_iters, snapshots, replicas.reshape(freqs, 2 * sensors, cands))
        log_power, band = pl.pallas_call(
            split_result,
            out_shape=(
                jax.ShapeDtypeStruct((freqs, HALF), F32),
                jax.ShapeDtypeStruct((1, HALF), F32),
            ),
            in_specs=[vmem],
            out_specs=(vmem, vmem),
            name="split",
        )(both)
        return log_power, band.reshape(HALF)

    return jax.shard_map(
        body,
        mesh=mesh,
        in_specs=(P("freq", "col", None), P("freq", None, "col", "row"), P("freq"), P("freq")),
        out_specs=(P("freq", ("row", "col")), P(("row", "col"))),
        check_vma=False,
    )
```

```python
import functools

import jax
import jax.numpy as jnp
from jax import lax
from jax.experimental import pallas as pl
from jax.experimental.pallas import tpu as pltpu
from jax.sharding import PartitionSpec as P

SENSORS = 1024
SNAPS = 64
LEVELS = 8
LANES = 128
HALF = 64
EXTRA = 8
WORDS = 80
GROUP = 16
FIELD = 20
TOP = 524287.0
GAIN_TARGET = 0.5
MESH_ID = pl.DeviceIdType.MESH
F32 = jnp.float32


def kernel(
    nf, nr, nz,
    lvl_hbm, it_hbm, snaps_hbm, reps_hbm,
    out_ref,
    lvl_ref, it_ref, snaps_ref, reps, part, part_n, first_w, first_n, recv_w, recv_n,
    gather, mat, gram, xsend, xrecv, gain, lsend, lrecv,
    in_sem, rs_s, rs_r, rn_s, rn_r, ga_s, ga_r, xx_s, xx_r, qz_s, qz_r, ll_s, ll_r,
):
    freqs = nr
    pairs = freqs // 2
    blocks = nr // 2
    hops = nz // 2
    me_f, me_r, me_z = lax.axis_index("freq"), lax.axis_index("row"), lax.axis_index("col")
    lane = lax.broadcasted_iota(jnp.int32, (1, LANES), 1)
    low = lane < HALF
    sign_hi = jnp.where(low, 1.0, -1.0).astype(F32)
    sign_lo = jnp.where(low, -1.0, 1.0).astype(F32)
    eye = lax.broadcasted_iota(jnp.int32, (HALF, LANES), 0) == lax.broadcasted_iota(jnp.int32, (HALF, LANES), 1)

    def swap(v):
        return pltpu.roll(v, HALF, 1)

    def ahead(me, step, count):
        return lax.rem(me + (step + count), count)

    def remote(src, dst, send, got, peer):
        return pltpu.make_async_remote_copy(
            src_ref=src, dst_ref=dst, send_sem=send, recv_sem=got, device_id=peer, device_id_type=MESH_ID,
        )

    barrier = pltpu.get_barrier_semaphore()
    greet = [("col", ahead(me_z, 1, nz)), ("col", ahead(me_z, -1, nz))]
    greet += [("row", ahead(me_r, o, nr)) for o in range(1, nr)]
    greet += [("freq", ahead(me_f, o, nf)) for o in range(1, nf)]
    for axis, peer in greet:
        pl.semaphore_signal(barrier, inc=1, device_id={axis: peer}, device_id_type=MESH_ID)

    small = []
    for i, (src, dst) in enumerate(((snaps_hbm, snaps_ref), (lvl_hbm, lvl_ref), (it_hbm, it_ref))):
        c = pltpu.make_async_copy(src, dst, in_sem.at[freqs + i])
        c.start()
        small.append(c)
    fetch = []
    for f in range(freqs):
        c = pltpu.make_async_copy(reps_hbm.at[f], reps.at[f], in_sem.at[f])
        c.start()
        fetch.append(c)

    for c in small:
        c.wait()

    for s in range(pairs):
        prods, norms = [], []
        for f in (s, s + pairs):
            fetch[f].wait()
            snap = snaps_ref[f].astype(F32)
            stacked = jnp.concatenate([snap * sign_hi, swap(snap)], axis=0)
            cols = reps[f]
            prods.append(jnp.dot(stacked.T.astype(jnp.bfloat16), cols, preferred_element_type=F32))
            wide = cols.astype(F32)
            norms.append(jnp.sum(wide * wide, axis=0, keepdims=True))
        for m in range(nz // 2):
            at = slice(m * LANES, (m + 1) * LANES)
            for pair, ref in ((prods, part), (norms, part_n)):
                a, b = pair[0][:, at], pair[1][:, at]
                ref[2 * m, s] = jnp.where(low, a, swap(b))
                ref[2 * m + 1, s] = jnp.where(low, swap(a), b)
    gather[me_z] = snaps_ref[me_r]

    def arm(s, way):
        return hops if (s < (pairs + 1) // 2) == (way == 0) else hops - 1

    def encode(v, ref):
        most = jnp.maximum(jnp.max(jnp.abs(v), axis=0, keepdims=True), 1e-30)
        q = jnp.round(v * (TOP / most)).astype(jnp.int32) & ((1 << FIELD) - 1)
        g = [q[i * GROUP:(i + 1) * GROUP] for i in range(8)]
        g_6, g_7 = g[6], g[7]
        tops = (
            g[5],
            lax.shift_right_logical(g[5], jnp.full((GROUP, LANES), 12, jnp.int32)) | (g_6 << 8),
            g_6 >> 4,
            (g_6 >> 16) | (g_7 << 4),
            g_7 >> 8,
        )
        for i, top in enumerate(tops):
            ref[i * GROUP:(i + 1) * GROUP, :] = g[i] | (top << FIELD)
        return most * (1.0 / TOP)

    def decode(ref, unit):
        w = ref[...]
        t = lax.shift_right_logical(w, jnp.full((WORDS, LANES), FIELD, jnp.int32))
        t = [t[i * GROUP:(i + 1) * GROUP] for i in range(5)]
        high = jnp.concatenate([
            t[0] | (t[1] << 12),
            (t[1] >> 8) | (t[2] << 4) | (t[3] << 16),
            (t[3] >> 4) | (t[4] << 8),
        ], axis=0)
        q = jnp.concatenate([w, high], axis=0)
        return ((q << (32 - FIELD)) >> (32 - FIELD)).astype(F32) * unit

    def target(way, t, s):
        return ahead(me_z, (1 if way == 0 else -1) * (arm(s, way) - t), nz)

    for s in range(pairs):
        for way in (0, 1):
            dest = target(way, 0, s)
            first_n[way, s, :1, :] = encode(part[dest, s], first_w.at[way, s])
            first_n[way, s, 1:, :] = part_n[dest, s]

    pl.semaphore_wait(barrier, len(greet))
    pending = []

    ring = {}

    def pass_on(h):
        for way, sign, reach in ((0, 1, hops), (1, -1, hops - 1)):
            if h < reach:
                slot = ahead(me_z, -sign * h, nz)
                if h == 0:
                    src = snaps_ref.at[me_r]
                else:
                    ring[way, h - 1].wait_recv()
                    src = gather.at[slot]
                c = remote(src, gather.at[slot], ga_s.at[way, h], ga_r.at[way, h], {"col": ahead(me_z, sign, nz)})
                c.start()
                ring[way, h] = c
                pending.append(c)

    found = {}

    def gram_done():
        ring[0, hops - 1].wait_recv()
        if hops > 1:
            ring[1, hops - 2].wait_recv()
        x = gather[...].reshape(nz * HALF, LANES)
        w = lax.dot_general(x, x, (((0,), (0,)), ((), ())), preferred_element_type=F32)
        gram[...] = (w[:HALF, :] + swap(w[HALF:, :]) * sign_hi) * (1.0 / SNAPS)
        diag = jnp.sum(jnp.where(eye, gram[...], 0.0), axis=0, keepdims=True)
        power = 2.0 * jnp.sum(diag, axis=1, keepdims=True) / (2.0 * SENSORS)
        level = lvl_ref[me_r]
        chosen = jnp.float32(0.0)
        for n in range(LEVELS):
            chosen = jnp.where(level == n, jnp.float32(2.0 ** (n / 2.0)), chosen)
        found["power"] = power
        found["load"] = chosen * power
        set_system(found["load"])

    def set_system(load):
        mat[...] = gram[...] + jnp.where(eye, load, 0.0)

    def sweep(first, last):
        def at(v, where):
            return jnp.sum(jnp.where(where, v, 0.0), axis=1, keepdims=True)

        def one(i, carry):
            k = 2 * i
            re0, re1 = lane == k, lane == k + 1
            im0, im1 = lane == k + HALF, lane == k + (HALF + 1)
            pivots = re0 | re1 | im0 | im1
            tile = mat[...]
            row0, row1 = mat[pl.ds(k, 1), :], mat[pl.ds(k + 1, 1), :]
            a, br, bi, c = at(row0, re0), at(row0, re1), at(row0, im1), at(row1, re1)
            c0r, c0i, c1r, c1i = at(tile, re0), at(tile, im0), at(tile, re1), at(tile, im1)
            r0 = jnp.where(re0, -1.0, jnp.where(pivots, 0.0, row0))
            r1 = jnp.where(re1, -1.0, jnp.where(pivots, 0.0, row1))
            j0, j1 = swap(r0) * sign_lo, swap(r1) * sign_lo
            inv = 1.0 / (a * c - (br * br + bi * bi))
            ca, cc, cr, ci = a * inv, c * inv, br * inv, bi * inv
            u0 = cc * r0 - (cr * r1 + ci * j1)
            u1 = ca * r1 - (cr * r0 - ci * j0)
            w0 = cc * j0 - (cr * j1 - ci * r1)
            w1 = ca * j1 - (cr * j0 + ci * r0)
            tile = jnp.where(pivots, 0.0, tile)
            mat[...] = tile - (c0r * u0 + c0i * w0) - (c1r * u1 + c1i * w1)
            mat[pl.ds(k, 1), :] = u0
            mat[pl.ds(k + 1, 1), :] = u1
            return carry

        twos = (last - first) // 2
        lax.fori_loop(0, twos, lambda i, carry: one(first + 2 * i + 1, one(first + 2 * i, carry)), 0)
        if (last - first) % 2:
            one(last - 1, 0)

    rs = {}

    def arrived(way, t, s):
        for c in rs[way, t, s]:
            c.wait_recv()
        n = recv_n[way, t, s]
        return decode(recv_w.at[way, t, s], n[:1]), n[1:]

    def send(way, t, s):
        if t == 0:
            words, norms = first_w.at[way, s], first_n.at[way, s]
        else:
            dest = target(way, t, s)
            more, more_n = arrived(way, t - 1, s)
            words, norms = recv_w.at[way, t - 1, s], recv_n.at[way, t - 1, s]
            norms[:1, :] = encode(part[dest, s] + more, words)
            norms[1:, :] = part_n[dest, s] + more_n
        to = {"col": ahead(me_z, 1 if way == 0 else -1, nz)}
        rs[way, t, s] = (
            remote(words, recv_w.at[way, t, s], rs_s.at[way, t, s], rs_r.at[way, t, s], to),
            remote(norms, recv_n.at[way, t, s], rn_s.at[way, t, s], rn_r.at[way, t, s], to),
        )
        for c in rs[way, t, s]:
            c.start()
            pending.append(c)

    half = (pairs + 1) // 2
    total_steps = hops * pairs
    gap = 3 if total_steps > 3 * hops + 4 else 1
    done = min(gap * (hops - 1) + 4, total_steps - 1)
    pivots = HALF // 2
    swept, share = 0, 3
    step = 0
    pass_on(0)
    next_hop = 1
    for t in range(hops):
        for s in range(pairs):
            if next_hop < hops and step >= gap * next_hop:
                pass_on(next_hop)
                next_hop += 1
            for way in (0, 1):
                turn = (s + way * half) % pairs
                if t < arm(turn, way):
                    send(way, t, turn)
            if step == done:
                while next_hop < hops:
                    pass_on(next_hop)
                    next_hop += 1
                gram_done()
            elif step > done:
                sweep(swept, swept + share)
                swept += share
            step += 1

    outgoing = {}
    for s in sorted(range(pairs), key=lambda s: s % half):
        total, norm = part[me_z, s], part_n[me_z, s]
        for way in (0, 1):
            more, more_n = arrived(way, arm(s, way) - 1, s)
            total, norm = total + more, norm + more_n
        up, down = total[:HALF], total[HALF:]
        for f, packed, row in (
            (s, jnp.where(low, up, swap(down)), norm),
            (s + pairs, jnp.where(low, swap(up), down), swap(norm)),
        ):
            xsend[f, :HALF, :] = packed
            xsend[f, HALF:, :] = jnp.broadcast_to(row, (EXTRA, LANES))
            c = remote(xsend.at[f], xrecv.at[me_r], xx_s.at[f], xx_r.at[me_r], {"row": f})
            outgoing[f] = c

            @pl.when(me_r != f)
            def _(c=c):
                c.start()

            @pl.when(me_r == f)
            def _(f=f):
                xrecv[f] = xsend[f]

    sweep(swept, pivots)
    for q in range(nr):
        @pl.when(me_r != q)
        def _(q=q):
            remote(xsend.at[q], xrecv.at[q], xx_s.at[q], xx_r.at[q], {"row": q}).wait_recv()

    proj, norm = [], []
    for m in range(blocks):
        a, b = xrecv[2 * m], xrecv[2 * m + 1]
        proj.append(jnp.concatenate([
            jnp.where(low, a[:HALF], swap(b[:HALF])),
            jnp.where(low, swap(a[:HALF]), b[:HALF]),
        ], axis=0) * (1.0 / 8.0))
        norm.append(jnp.where(low, a[HALF:HALF + 1], swap(b[HALF:HALF + 1])))
    proj = jnp.concatenate(proj, axis=1)
    norm = jnp.concatenate(norm, axis=1)

    def solve():
        inverse = -mat[...]
        full = jnp.concatenate([inverse * sign_hi, swap(inverse)], axis=0)
        return jnp.dot(full, proj, precision=lax.Precision.HIGHEST, preferred_element_type=F32)

    z = solve()
    inner = jnp.sum(proj * z, axis=0, keepdims=True)
    energy = jnp.sum(z * z, axis=0, keepdims=True)
    load_one = found["load"]
    first_quad = (norm - inner) / load_one
    quad_two = (first_quad - energy) / load_one
    gains = first_quad * first_quad / (quad_two * norm)
    mine = jnp.sum(gains, axis=1, keepdims=True)

    gain[me_z] = jnp.broadcast_to(mine, (1, LANES))
    copies = []
    for o in sorted(range(1, nz), key=lambda o: abs(o - hops)):
        c = remote(gain.at[me_z], gain.at[me_z], qz_s.at[o], qz_r.at[o], {"col": ahead(me_z, o, nz)})
        c.start()
        copies.append(c)
    for c in copies:
        c.wait_recv()
    pending.extend(copies)
    whole = gain[0]
    for i in range(1, nz):
        whole = whole + gain[i]
    mean_gain = whole / (HALF * nz * nr)
    ratio = GAIN_TARGET / mean_gain[:, :1]
    load_two = load_one * (1.0 + ratio * ratio)
    set_system(load_two)
    sweep(0, pivots)

    z = solve()
    quad_next = (norm - jnp.sum(proj * z, axis=0, keepdims=True)) / load_two
    final = jnp.where(it_ref[me_r] >= 2, quad_next, first_quad)
    log_power = jnp.log(norm / (final * found["power"]))
    for m in range(blocks):
        block = log_power[:, m * LANES:(m + 1) * LANES]
        lsend[2 * m] = block
        lsend[2 * m + 1] = swap(block)

    lrecv[me_f, me_r] = lsend[me_r]
    copies = []
    for of in sorted(range(nf), key=lambda o: abs(o - nf // 2)):
        for o in sorted(range(nr), key=lambda o: abs(o - nr // 2)):
            if of or o:
                to_f, to_r = ahead(me_f, of, nf), ahead(me_r, o, nr)
                c = remote(lsend.at[to_r], lrecv.at[me_f, me_r], ll_s.at[of, o], ll_r.at[of, o], {"freq": to_f, "row": to_r})
                c.start()
                copies.append(c)
    for c in copies:
        c.wait_recv()
    pending.extend(copies)
    band = jnp.zeros((1, LANES), F32)
    for f in range(nf):
        for r in range(nr):
            band = band + lrecv[f, r]
    for r in range(nr):
        out_ref[r:r + 1, :] = lrecv[me_f, r]
    out_ref[nr:, :] = jnp.broadcast_to(band / (freqs * nf), (EXTRA, LANES))

    for c in pending:
        c.wait_send()
    for f in range(freqs):
        @pl.when(me_r != f)
        def _(f=f):
            outgoing[f].wait_send()


def split_result(both_ref, logp_ref, band_ref):
    rows = logp_ref.shape[0]
    logp_ref[...] = both_ref[:rows, :HALF]
    band_ref[...] = both_ref[rows:rows + 1, :HALF]


def solution(mesh):
    nf, nr, nz = mesh.shape["freq"], mesh.shape["row"], mesh.shape["col"]
    pairs, hops = nr // 2, nz // 2
    dma = pltpu.SemaphoreType.DMA

    def body(snapshots, replicas, level_index, loading_iters):
        freqs, sensors, cands = snapshots.shape[0], snapshots.shape[1], replicas.shape[3]
        vmem = pl.BlockSpec(memory_space=pltpu.VMEM)
        both = pl.pallas_call(
            functools.partial(kernel, nf, nr, nz),
            out_shape=jax.ShapeDtypeStruct((freqs + EXTRA, LANES), F32),
            in_specs=[pl.BlockSpec(memory_space=pl.ANY)] * 4,
            out_specs=vmem,
            scratch_shapes=[
                pltpu.SMEM((freqs,), jnp.int32),
                pltpu.SMEM((freqs,), jnp.int32),
                pltpu.VMEM((freqs, sensors, LANES), jnp.bfloat16),
                pltpu.VMEM((freqs, 2 * sensors, cands), jnp.bfloat16),
                pltpu.VMEM((nz, pairs, LANES, LANES), F32),
                pltpu.VMEM((nz, pairs, 1, LANES), F32),
                pltpu.VMEM((2, pairs, WORDS, LANES), jnp.int32),
                pltpu.VMEM((2, pairs, 2, LANES), F32),
                pltpu.VMEM((2, hops, pairs, WORDS, LANES), jnp.int32),
                pltpu.VMEM((2, hops, pairs, 2, LANES), F32),
                pltpu.VMEM((nz, sensors, LANES), jnp.bfloat16),
                pltpu.VMEM((HALF, LANES), F32),
                pltpu.VMEM((HALF, LANES), F32),
                pltpu.VMEM((nr, HALF + EXTRA, LANES), F32),
                pltpu.VMEM((nr, HALF + EXTRA, LANES), F32),
                pltpu.VMEM((nz, 1, LANES), F32),
                pltpu.VMEM((nr, 1, LANES), F32),
                pltpu.VMEM((nf, nr, 1, LANES), F32),
                dma((freqs + 3,)),
                dma((2, hops, pairs)), dma((2, hops, pairs)),
                dma((2, hops, pairs)), dma((2, hops, pairs)),
                dma((2, hops)), dma((2, hops)),
                dma((nr,)), dma((nr,)),
                dma((nz,)), dma((nz,)),
                dma((nf, nr)), dma((nf, nr)),
            ],
            compiler_params=pltpu.CompilerParams(collective_id=0, has_side_effects=True),
            name="mvdr",
        )(level_index, loading_iters, snapshots, replicas.reshape(freqs, 2 * sensors, cands))
        log_power, band = pl.pallas_call(
            split_result,
            out_shape=(
                jax.ShapeDtypeStruct((freqs, HALF), F32),
                jax.ShapeDtypeStruct((1, HALF), F32),
            ),
            in_specs=[vmem],
            out_specs=(vmem, vmem),
            name="split",
        )(both)
        return log_power, band.reshape(HALF)

    return jax.shard_map(
        body,
        mesh=mesh,
        in_specs=(P("freq", "col", None), P("freq", None, "col", "row"), P("freq"), P("freq")),
        out_specs=(P("freq", ("row", "col")), P(("row", "col"))),
        check_vma=False,
    )
```
